16 devices in a mesh: dp: 4 (over y, z, core), tp: 4 (over x).
Axes of the slice: x: 4, y: 2, z: 1, core: 2. Of those that a mesh axis runs over, the one named last changes fastest.
The devices are a block of a 4x4x8 slice.
Arguments:
- x: bfloat16 [8192, 2048], P('dp'), parts along dimension 0
- dy: bfloat16 [8192, 2048], P('dp'), parts along dimension 0
- gate: bfloat16 [8192, 5632], P('dp', 'tp'), parts along dimension 0
- up: bfloat16 [8192, 5632], P('dp', 'tp'), parts along dimension 0
- w_gate: bfloat16 [2048, 5632], P(None, 'tp')
- w_up: bfloat16 [2048, 5632], P(None, 'tp')
- w_down: bfloat16 [5632, 2048], P('tp')
Outputs:
- output 1: bfloat16 [8192, 2048], P('dp'), parts along dimension 0
- output 2: bfloat16 [8192, 5632], P('dp', 'tp'), parts along dimension 0
- output 3: bfloat16 [8192, 5632], P('dp', 'tp'), parts along dimension 0
- output 4: bfloat16 [22528, 2048], P(('dp', 'tp')), parts along dimension 0
There are 4 independent parts. The reference program is written for one: setup_inputs(seed, part) draws one part's arguments, and reference() takes and returns one part's arrays. A program takes and returns all parts, laid end to end along the dimension named above; an argument that names none is the same for every part.
All inputs are finite; a program needn't handle non-finite values.
Results may differ from the reference program's by a relative error of at most 0.012.
Values are sent between devices in bfloat16 or wider.
A program may use at most 768 MiB of HBM per device.

```python
import jax
import jax.numpy as jnp

ROWS = 2048
D = 2048
FF = 5632


def act(gate, up):
    return jax.nn.silu(gate) * up


def setup_inputs(seed: int = 0, part: int = 0) -> dict:
    kx, ky, ka, kb, kg, ku, kd = jax.random.split(jax.random.key(seed), 7)
    kx, ky, ka, kb = (jax.random.fold_in(k, part) for k in (kx, ky, ka, kb))
    drawn = {
        "x": jax.random.normal(kx, (ROWS, D), jnp.float32),
        "dy": jax.random.normal(ky, (ROWS, D), jnp.float32),
        "gate": jax.random.normal(ka, (ROWS, FF), jnp.float32),
        "up": jax.random.normal(kb, (ROWS, FF), jnp.float32),
        "w_gate": jax.random.normal(kg, (D, FF), jnp.float32) * D**-0.5,
        "w_up": jax.random.normal(ku, (D, FF), jnp.float32) * D**-0.5,
        "w_down": jax.random.normal(kd, (FF, D), jnp.float32) * FF**-0.5,
    }
    return {k: v.astype(jnp.bfloat16) for k, v in drawn.items()}


def reference(x, dy, gate, up, w_gate, w_up, w_down):
    hidden, back = jax.vjp(act, gate.astype(jnp.float32), up.astype(jnp.float32))
    d_hidden = jnp.dot(dy, w_down.T, preferred_element_type=jnp.float32)
    d_gate, d_up = (g.astype(jnp.bfloat16) for g in back(d_hidden))
    dx = jnp.dot(d_gate, w_gate.T, preferred_element_type=jnp.float32) + jnp.dot(d_up, w_up.T, preferred_element_type=jnp.float32)
    dw_gate = jnp.dot(x.T, d_gate, preferred_element_type=jnp.float32)
    dw_up = jnp.dot(x.T, d_up, preferred_element_type=jnp.float32)
    dw_down = jnp.dot(hidden.astype(jnp.bfloat16).T, dy, preferred_element_type=jnp.float32)
    return tuple(g.astype(jnp.bfloat16) for g in (dx, dw_gate, dw_up, dw_down))
```

```python
import functools

import jax
import jax.numpy as jnp
from jax import lax
from jax.experimental import pallas as pl
from jax.experimental.pallas import tpu as pltpu
from jax.sharding import PartitionSpec as P

F32, BF16 = jnp.float32, jnp.bfloat16
ANY = pl.BlockSpec(memory_space=pl.ANY)
NT = (((1,), (1,)), ((), ()))
TN = (((0,), (0,)), ((), ()))
SUB = 4


def dot(a, b, dims):
    return lax.dot_general(a, b, dims, preferred_element_type=F32)


def reduce_kernel(n, dy, gate, up, w_gate, w_up, w_down, mine, d_cat, hidden,
                  wd_v, wc_v, dy_v, g_v, u_v, dc_v, h_v, buf,
                  w_sem, in_sem, out_sem, send_sem, recv_sem, mine_sem):
    me = lax.axis_index("tp")
    half, width, ff = dy_v.shape[1], buf.shape[-1], g_v.shape[-1]

    def rows_of(s, d):
        block = lax.rem(me + (2 * d - 1) * (s + 1) + 2 * n, n)
        return pl.multiple_of((2 * block + d) * half, half)

    def load(k):
        rows = pl.ds(rows_of(k // 2, lax.rem(k, 2)), half)
        slot = lax.rem(k, 2)
        return [
            pltpu.make_async_copy(dy.at[rows], dy_v.at[slot], in_sem.at[0, slot]),
            pltpu.make_async_copy(gate.at[rows], g_v.at[slot], in_sem.at[1, slot]),
            pltpu.make_async_copy(up.at[rows], u_v.at[slot], in_sem.at[2, slot]),
        ]

    def save(k):
        rows = pl.ds(rows_of(k // 2, lax.rem(k, 2)), half)
        slot = lax.rem(k, 2)
        return [
            pltpu.make_async_copy(dc_v.at[slot], d_cat.at[rows], out_sem.at[0, slot]),
            pltpu.make_async_copy(h_v.at[slot], hidden.at[rows], out_sem.at[1, slot]),
        ]

    def weight(c):
        rows = pl.ds(pl.multiple_of(c * width, width), width)
        return [
            pltpu.make_async_copy(w_gate.at[rows], wc_v.at[rows, pl.ds(0, ff)], w_sem.at[1 + 2 * c]),
            pltpu.make_async_copy(w_up.at[rows], wc_v.at[rows, pl.ds(ff, ff)], w_sem.at[2 + 2 * c]),
        ]

    def hop(s, d, c):
        return pltpu.make_async_remote_copy(
            src_ref=buf.at[s, d, c],
            dst_ref=buf.at[s + 1, d, c],
            send_sem=send_sem.at[s, d, c],
            recv_sem=recv_sem.at[s, d, c],
            device_id={"tp": lax.rem(me + 1 - 2 * d + n, n)},
            device_id_type=pl.DeviceIdType.MESH,
        )

    def keep(d, c):
        rows = pl.ds(pl.multiple_of(d * half, half), half)
        cols = pl.ds(pl.multiple_of(c * width, width), width)
        return pltpu.make_async_copy(buf.at[n - 1, d, c], mine.at[rows, cols], mine_sem.at[d, c])

    copy_wd = pltpu.make_async_copy(w_down, wd_v, w_sem.at[0])
    first = load(0)
    first[0].start()
    copy_wd.start()
    for copy in first[1:] + weight(0) + load(1):
        copy.start()
    for c in range(1, SUB):
        for copy in weight(c):
            copy.start()

    barrier = pltpu.get_barrier_semaphore()
    for step in (1, n - 1):
        pl.semaphore_signal(barrier, inc=1, device_id={"tp": lax.rem(me + step, n)}, device_id_type=pl.DeviceIdType.MESH)
    buf[0] = jnp.zeros(buf.shape[1:], BF16)
    pl.semaphore_wait(barrier, 2)
    copy_wd.wait()

    def grads(k):
        slot = lax.rem(k, 2)
        for copy in load(k):
            copy.wait()

        @pl.when(k >= 2)
        def _():
            for copy in save(k - 2):
                copy.wait()

        for f in range(0, ff, 256):
            cols = pl.ds(f, min(256, ff - f))
            dh = dot(dy_v[slot], wd_v[cols, :], NT)
            g, u = g_v[slot, :, cols].astype(F32), u_v[slot, :, cols].astype(F32)
            sig = jax.nn.sigmoid(g)
            silu = g * sig
            h_v[slot, :, cols] = (silu * u).astype(BF16)
            dc_v[slot, :, cols] = (dh * u * (sig * (1.0 + g * (1.0 - sig)))).astype(BF16)
            dc_v[slot, :, pl.ds(ff + f, min(256, ff - f))] = (dh * silu).astype(BF16)
        for copy in save(k):
            copy.start()

        @pl.when(k + 2 < 2 * n)
        def _():
            for copy in load(k + 2):
                copy.start()

    def term(s, d, c):
        @pl.when((s == 0) & (d == 0))
        def _():
            for copy in weight(c):
                copy.wait()

        @pl.when(s > 0)
        def _():
            hop(s - 1, d, c).wait_recv()

        cols = pl.ds(pl.multiple_of(c * width, width), width)
        acc = dot(dc_v[d], wc_v[cols, :], NT)
        buf[s, d, c] = (acc + buf[s, d, c].astype(F32)).astype(BF16)

        @pl.when(s < n - 1)
        def _():
            hop(s, d, c).start()

        @pl.when(s == n - 1)
        def _():
            keep(d, c).start()

    def step(s, _):
        def lead(d, _):
            grads(2 * s + d)
            term(s, d, 0)
            return 0

        def rest(q, _):
            term(s, lax.rem(q, 2), q // 2)
            return 0

        lax.fori_loop(0, 2, lead, 0)
        lax.fori_loop(2, 2 * SUB, rest, 0)
        return 0

    lax.fori_loop(0, n, step, 0)

    def drain(s, _):
        for d in range(2):
            for c in range(SUB):
                hop(s, d, c).wait_send()
        return 0

    lax.fori_loop(0, n - 1, drain, 0)
    for d in range(2):
        for copy in save(2 * n - 2 + d):
            copy.wait()
        for c in range(SUB):
            keep(d, c).wait()


def reduce_terms(n, dy, gate, up, w_gate, w_up, w_down):
    (rows, d), ff = dy.shape, gate.shape[1]
    half, width = rows // (2 * n), d // SUB
    sems = pltpu.SemaphoreType.DMA
    return pl.pallas_call(
        functools.partial(reduce_kernel, n),
        out_shape=[
            jax.ShapeDtypeStruct((rows // n, d), BF16),
            jax.ShapeDtypeStruct((rows, 2 * ff), BF16),
            jax.ShapeDtypeStruct((rows, ff), BF16),
        ],
        in_specs=[ANY] * 6,
        out_specs=[ANY] * 3,
        scratch_shapes=[
            pltpu.VMEM((ff, d), BF16),
            pltpu.VMEM((d, 2 * ff), BF16),
            pltpu.VMEM((2, half, d), BF16),
            pltpu.VMEM((2, half, ff), BF16),
            pltpu.VMEM((2, half, ff), BF16),
            pltpu.VMEM((2, half, 2 * ff), BF16),
            pltpu.VMEM((2, half, ff), BF16),
            pltpu.VMEM((n, 2, SUB, half, width), BF16),
            sems((1 + 2 * SUB,)),
            sems((3, 2)),
            sems((2, 2)),
            sems((n - 1, 2, SUB)),
            sems((n - 1, 2, SUB)),
            sems((2, SUB)),
        ],
        compiler_params=pltpu.CompilerParams(
            collective_id=0, has_side_effects=True, vmem_limit_bytes=60 * 2**20
        ),
        cost_estimate=pl.CostEstimate(flops=6 * rows * d * ff, bytes_accessed=8 * rows * d, transcendentals=2 * rows * ff),
        name="reduce_terms",
    )(dy, gate, up, w_gate, w_up, w_down)


def grad_kernel(a, b, out):
    out[...] = dot(a[...], b[...], TN).astype(BF16)


def weight_grad(a, b, b_cols=None, b_start=0, tile=256):
    tokens, m = a.shape
    b_cols = b_cols or b.shape[1]
    return pl.pallas_call(
        grad_kernel,
        out_shape=jax.ShapeDtypeStruct((m, b_cols), BF16),
        grid=(m // tile,),
        in_specs=[
            pl.BlockSpec((tokens, tile), lambda i: (0, i)),
            pl.BlockSpec((tokens, b_cols), lambda i: (0, b_start), pipeline_mode=pl.Buffered(1)),
        ],
        out_specs=pl.BlockSpec((tile, b_cols), lambda i: (i, 0)),
        compiler_params=pltpu.CompilerParams(vmem_limit_bytes=48 * 2**20),
        cost_estimate=pl.CostEstimate(
            flops=2 * tokens * m * b_cols, bytes_accessed=2 * (tokens * (m + b_cols) + m * b_cols), transcendentals=0
        ),
        name="weight_grad",
    )(a, b)


def solution(mesh):
    n = mesh.shape["tp"]

    def step(x, dy, gate, up, w_gate, w_up, w_down):
        ff = gate.shape[1]
        mine, d_cat, hidden = reduce_terms(n, dy, gate, up, w_gate, w_up, w_down)
        dx = lax.all_gather(mine, "tp", tiled=True)
        dw_gate = weight_grad(x, d_cat, ff, 0)
        dw_up = weight_grad(x, d_cat, ff, 1)
        dw_down = weight_grad(hidden, dy, tile=128)
        return dx, dw_gate, dw_up, dw_down

    tokens, columns, rows = P("dp", None), P(None, "tp"), P("tp", None)
    return jax.shard_map(
        step,
        mesh=mesh,
        in_specs=(tokens, tokens, P("dp", "tp"), P("dp", "tp"), columns, columns, rows),
        out_specs=(tokens, P("dp", "tp"), P("dp", "tp"), P(("dp", "tp"), None)),
        check_vma=False,
    )
```

```python
import functools

import jax
import jax.numpy as jnp
from jax import lax
from jax.experimental import pallas as pl
from jax.experimental.pallas import tpu as pltpu
from jax.sharding import PartitionSpec as P

F32, BF16 = jnp.float32, jnp.bfloat16
MIB = 2**20
ANY = pl.BlockSpec(memory_space=pl.ANY)
NT = (((1,), (1,)), ((), ()))
NN = (((1,), (0,)), ((), ()))
TN = (((0,), (0,)), ((), ()))
PARTS = 2
SUB = 4
TILE = 256


def dot(a, b, dims):
    return lax.dot_general(a, b, dims, preferred_element_type=F32)


def ring_kernel(n, x, dy, gate, up, w_gate, w_up, w_down,
                dx, last_0, last_1, hidden_t, dw_gate, dw_up,
                wd_v, wc_v, dy_v, g_v, u_v, h_v, dc_v, buf, ag, x_v, xt_v, dw_v,
                wd_sem, wc_sem, in_sem, h_sem, send_sem, recv_sem, gsend_sem, grecv_sem, keep_sem, last_sem,
                x_sem, dw_sem):
    me = lax.axis_index("tp")
    piece, width, ff = buf.shape[4], buf.shape[5], g_v.shape[-1]
    half = PARTS * piece
    chunks, messages, tiles = n * PARTS, PARTS * SUB, x.shape[1] // TILE

    def block_row(block, d, h):
        return pl.multiple_of((2 * lax.rem(block + 2 * n, n) + d) * half + h * piece, piece)

    def row_of(k, d):
        return block_row(me + (2 * d - 1) * (k // PARTS + 1), d, lax.rem(k, PARTS))

    def load(k):
        slot = lax.rem(k, 2)
        return [
            pltpu.make_async_copy(src.at[pl.ds(row_of(k, d), piece)], dst.at[slot, pl.ds(d * piece, piece)], in_sem.at[i, d, slot])
            for d in range(2)
            for i, (src, dst) in enumerate(((dy, dy_v), (gate, g_v), (up, u_v)))
        ]

    def save(k):
        slot = lax.rem(k, 2)
        return [
            pltpu.make_async_copy(h_v.at[slot, :, pl.ds(d * piece, piece)], hidden_t.at[:, pl.ds(row_of(k, d), piece)], h_sem.at[d, slot])
            for d in range(2)
        ]

    def down(f):
        rows = pl.ds(f, min(TILE, ff - f))
        return pltpu.make_async_copy(w_down.at[rows], wd_v.at[rows], wd_sem.at[f // TILE])

    def weight(c):
        rows = pl.ds(pl.multiple_of(c * width, width), width)
        return [
            pltpu.make_async_copy(w_gate.at[rows], wc_v.at[rows, pl.ds(0, ff)], wc_sem.at[0, c]),
            pltpu.make_async_copy(w_up.at[rows], wc_v.at[rows, pl.ds(ff, ff)], wc_sem.at[1, c]),
        ]

    def to(d):
        return {"device_id": {"tp": lax.rem(me + 1 - 2 * d + n, n)}, "device_id_type": pl.DeviceIdType.MESH}

    def hop(s, h, c, d):
        return pltpu.make_async_remote_copy(
            src_ref=buf.at[s, h, c, d], dst_ref=buf.at[s + 1, h, c, d],
            send_sem=send_sem.at[s, h, c, d], recv_sem=recv_sem.at[s, h, c, d], **to(d),
        )

    def spread(r, h, c, d):
        return pltpu.make_async_remote_copy(
            src_ref=buf.at[n - 1, h, c, d] if r == 0 else ag.at[r - 1, h, c, d], dst_ref=ag.at[r, h, c, d],
            send_sem=gsend_sem.at[r, h, c, d], recv_sem=grecv_sem.at[r, h, c, d], **to(d),
        )

    def keep(r, h, c, d):
        cols = pl.ds(pl.multiple_of(c * width, width), width)
        return pltpu.make_async_copy(
            buf.at[n - 1, h, c, d] if r == 0 else ag.at[r - 1, h, c, d],
            dx.at[pl.ds(block_row(me + (2 * d - 1) * r, d, h), piece), cols], keep_sem.at[r, h, c, d],
        )

    def hand(h, c, d):
        cols = pl.ds(pl.multiple_of(c * width, width), width)
        return pltpu.make_async_copy(
            ag.at[n - 3, h, c, d], (last_0, last_1)[d].at[pl.ds(pl.multiple_of(h * piece, piece), piece), cols], last_sem.at[h, c, d]
        )

    def load_x(j):
        cols = pl.ds(pl.multiple_of(j * TILE, TILE), TILE)
        slot = lax.rem(j, 2)
        return pltpu.make_async_copy(x.at[:, cols], x_v.at[slot], x_sem.at[slot])

    def save_dw(j):
        rows = pl.ds(pl.multiple_of(j * TILE, TILE), TILE)
        slot = lax.rem(j, 2)
        return [
            pltpu.make_async_copy(dw_v.at[slot, :, pl.ds(0, ff)], dw_gate.at[rows], dw_sem.at[0, slot]),
            pltpu.make_async_copy(dw_v.at[slot, :, pl.ds(ff, ff)], dw_up.at[rows], dw_sem.at[1, slot]),
        ]

    def start(copies):
        for copy in copies:
            copy.start()

    def wait(copies):
        for copy in copies:
            copy.wait()

    f_tiles = range(0, ff, TILE)
    now = load(0)
    start(now[::3])
    start([down(f) for f in f_tiles])
    start(now[1:3] + now[4:] + weight(0))

    barrier = pltpu.get_barrier_semaphore()
    for d in range(2):
        pl.semaphore_signal(barrier, inc=1, **to(d))
    buf[0] = jnp.zeros(buf.shape[1:], BF16)
    pl.semaphore_wait(barrier, 2)

    def grads(k, first=False):
        slot = lax.rem(k, 2)
        wait(load(k))
        if not first:
            @pl.when(k >= 2)
            def _():
                wait(save(k - 2))

        for f in f_tiles:
            size = min(TILE, ff - f)
            cols = pl.ds(f, size)
            if first:
                down(f).wait()
            dh = dot(dy_v[slot], wd_v[cols, :], NT)
            g, u = g_v[slot, :, cols].astype(F32), u_v[slot, :, cols].astype(F32)
            sig = jax.nn.sigmoid(g)
            silu = g * sig
            h_v[slot, cols, :] = (silu * u).astype(BF16).T
            d_gate = (dh * u * (sig * (1.0 + g * (1.0 - sig)))).astype(BF16)
            d_up = (dh * silu).astype(BF16)
            for d in range(2):
                rows = pl.ds(row_of(k, d), piece)
                dc_v[rows, cols] = d_gate[d * piece:(d + 1) * piece]
                dc_v[rows, pl.ds(ff + f, size)] = d_up[d * piece:(d + 1) * piece]
        start(save(k))

        @pl.when(k + 2 < chunks)
        def _():
            start(load(k + 2))

    def term(k, c, first=False):
        s, h = k // PARTS, lax.rem(k, PARTS)
        if first:
            wait(weight(c))

        @pl.when(s > 0)
        def _():
            for d in range(2):
                hop(s - 1, h, c, d).wait_recv()

        cols = pl.ds(pl.multiple_of(c * width, width), width)
        rows = [dc_v[pl.ds(row_of(k, d), piece), :] for d in range(2)]
        acc = dot(jnp.concatenate(rows, axis=0), wc_v[cols, :], NT)
        for d in range(2):
            own = acc[d * piece:(d + 1) * piece]
            buf[s, h, c, d] = (own + buf[s, h, c, d].astype(F32)).astype(BF16)

        @pl.when(s < n - 1)
        def _():
            for d in range(2):
                hop(s, h, c, d).start()

        @pl.when(s == n - 1)
        def _():
            for d in range(2):
                spread(0, h, c, d).start()
                keep(0, h, c, d).start()

    grads(0, first=True)
    for c in range(1, SUB):
        start(weight(c))
    start(load(1))

    def term0(c, _):
        term(0, c, first=True)
        return 0

    lax.fori_loop(0, SUB, term0, 0)

    def chunk(k, _):
        grads(k)

        def terms(c, _):
            term(k, c)
            return 0

        lax.fori_loop(0, SUB, terms, 0)
        return 0

    start([load_x(0), load_x(1)])
    lax.fori_loop(1, chunks, chunk, 0)

    def forward(r, m):
        h, c = m // SUB, lax.rem(m, SUB)
        for d in range(2):
            spread(r - 1, h, c, d).wait_recv()
            keep(r, h, c, d).start()
            if r < n - 2:
                spread(r, h, c, d).start()
            else:
                hand(h, c, d).start()

    per = -(-messages * (n - 3) // tiles)

    def tile(j, _):
        slot = lax.rem(j, 2)
        load_x(j).wait()
        xt_v[...] = x_v[slot].T

        @pl.when(j >= 2)
        def _():
            wait(save_dw(j - 2))

        for f in range(0, 2 * ff, 2 * TILE):
            cols = pl.ds(f, min(2 * TILE, 2 * ff - f))
            dw_v[slot, :, cols] = dot(xt_v[...], dc_v[:, cols], NN).astype(BF16)
        start(save_dw(j))

        @pl.when(j + 2 < tiles)
        def _():
            load_x(j + 2).start()

        for r in range(1, n - 2):
            for i in range(per):
                m = j * per + i

                @pl.when(m < messages)
                def _():
                    forward(r, m)
        return 0

    lax.fori_loop(0, tiles, tile, 0)

    def arrive(m, _):
        forward(n - 2, m)
        return 0

    lax.fori_loop(0, messages, arrive, 0)

    def drain(m, _):
        h, c = m // SUB, lax.rem(m, SUB)
        for d in range(2):
            for s in range(n - 1):
                hop(s, h, c, d).wait_send()
            for r in range(n - 2):
                spread(r, h, c, d).wait_send()
            for r in range(n - 1):
                keep(r, h, c, d).wait()
            hand(h, c, d).wait()
        return 0

    lax.fori_loop(0, messages, drain, 0)
    for k in range(chunks - 2, chunks):
        wait(save(k))
    for j in range(tiles - 2, tiles):
        wait(save_dw(j))


def ring(n, x, dy, gate, up, w_gate, w_up, w_down):
    (rows, d), ff = dy.shape, gate.shape[1]
    piece, width = rows // (2 * n * PARTS), d // SUB
    dma = pltpu.SemaphoreType.DMA
    each = (PARTS, SUB, 2)
    return pl.pallas_call(
        functools.partial(ring_kernel, n),
        out_shape=[
            jax.ShapeDtypeStruct((rows, d), BF16),
            jax.ShapeDtypeStruct((PARTS * piece, d), BF16),
            jax.ShapeDtypeStruct((PARTS * piece, d), BF16),
            jax.ShapeDtypeStruct((ff, rows), BF16),
            jax.ShapeDtypeStruct((d, ff), BF16),
            jax.ShapeDtypeStruct((d, ff), BF16),
        ],
        in_specs=[ANY] * 7,
        out_specs=[ANY] * 6,
        scratch_shapes=[
            pltpu.VMEM((ff, d), BF16),
            pltpu.VMEM((d, 2 * ff), BF16),
            pltpu.VMEM((2, 2 * piece, d), BF16),
            pltpu.VMEM((2, 2 * piece, ff), BF16),
            pltpu.VMEM((2, 2 * piece, ff), BF16),
            pltpu.VMEM((2, ff, 2 * piece), BF16),
            pltpu.VMEM((rows, 2 * ff), BF16),
            pltpu.VMEM((n, *each, piece, width), BF16),
            pltpu.VMEM((n - 2, *each, piece, width), BF16),
            pltpu.VMEM((2, rows, TILE), BF16),
            pltpu.VMEM((TILE, rows), BF16),
            pltpu.VMEM((2, TILE, 2 * ff), BF16),
            dma((-(-ff // TILE),)),
            dma((2, SUB)),
            dma((3, 2, 2)),
            dma((2, 2)),
            dma((n - 1, *each)),
            dma((n - 1, *each)),
            dma((n - 2, *each)),
            dma((n - 2, *each)),
            dma((n - 1, *each)),
            dma(each),
            dma((2,)),
            dma((2, 2)),
        ],
        compiler_params=pltpu.CompilerParams(
            collective_id=0, has_side_effects=True, vmem_limit_bytes=62 * MIB
        ),
        cost_estimate=pl.CostEstimate(flops=10 * rows * d * ff, bytes_accessed=16 * rows * d, transcendentals=2 * rows * ff),
        name="ring",
    )(x, dy, gate, up, w_gate, w_up, w_down)


def finish_kernel(places, hidden_t, dy, dx_in, dw_gate_in, dw_up_in, dw_down, dx, dw_gate, dw_up):
    del places
    dx[...] = dx_in[...]
    dw_gate[...] = dw_gate_in[...]
    dw_up[...] = dw_up_in[...]
    dw_down[...] = dot(hidden_t[...], dy[...], NN).astype(BF16)


def finish(n, dx, hidden_t, dy, dw_gate, dw_up):
    (rows, d), ff = dy.shape, hidden_t.shape[0]
    half, steps = rows // (2 * n), d // TILE
    me = lax.axis_index("tp")
    step = jnp.minimum(jnp.arange(steps), 2 * n - 3)
    way = step % 2
    places = 2 * ((me + (2 * way - 1) * (step // 2) + n) % n) + way
    here = lambda j, p: (j, 0)
    place = lambda j, p: (p[j], 0)
    return pl.pallas_call(
        finish_kernel,
        out_shape=[
            jax.ShapeDtypeStruct((ff, d), BF16),
            jax.ShapeDtypeStruct((rows, d), BF16),
            jax.ShapeDtypeStruct((d, ff), BF16),
            jax.ShapeDtypeStruct((d, ff), BF16),
        ],
        grid_spec=pltpu.PrefetchScalarGridSpec(
            num_scalar_prefetch=1,
            grid=(steps,),
            in_specs=[
                pl.BlockSpec((ff, rows), lambda j, p: (0, 0), pipeline_mode=pl.Buffered(1)),
                pl.BlockSpec((rows, TILE), lambda j, p: (0, j)),
                pl.BlockSpec((half, d), place),
                pl.BlockSpec((TILE, ff), here),
                pl.BlockSpec((TILE, ff), here),
            ],
            out_specs=[
                pl.BlockSpec((ff, TILE), lambda j, p: (0, j)),
                pl.BlockSpec((half, d), place),
                pl.BlockSpec((TILE, ff), here),
                pl.BlockSpec((TILE, ff), here),
            ],
        ),
        compiler_params=pltpu.CompilerParams(vmem_limit_bytes=62 * MIB),
        cost_estimate=pl.CostEstimate(flops=2 * rows * d * ff, bytes_accessed=12 * rows * d, transcendentals=0),
        name="finish",
    )(places, hidden_t, dy, dx, dw_gate, dw_up)


def solution(mesh):
    n = mesh.shape["tp"]

    def step(x, dy, gate, up, w_gate, w_up, w_down):
        me, half = lax.axis_index("tp"), x.shape[0] // (2 * n)
        dx, *last, hidden_t, dw_gate, dw_up = ring(n, x, dy, gate, up, w_gate, w_up, w_down)
        ends = [lax.ppermute(last[d], "tp", [(i, (i + 1 - 2 * d) % n) for i in range(n)]) for d in range(2)]
        dw_down, dx, dw_gate, dw_up = finish(n, dx, hidden_t, dy, dw_gate, dw_up)
        for d in range(2):
            block = lax.rem(me + (2 * d - 1) * (n - 1) + n, n)
            dx = lax.dynamic_update_slice(dx, ends[d], ((2 * block + d) * half, 0))
        return dx, dw_gate, dw_up, dw_down

    tokens, columns, rows = P("dp", None), P(None, "tp"), P("tp", None)
    return jax.shard_map(
        step,
        mesh=mesh,
        in_specs=(tokens, tokens, P("dp", "tp"), P("dp", "tp"), columns, columns, rows),
        out_specs=(tokens, P("dp", "tp"), P("dp", "tp"), P(("dp", "tp"), None)),
        check_vma=False,
    )
```

```python
import functools

import jax
import jax.numpy as jnp
from jax import lax
from jax.experimental import pallas as pl
from jax.experimental.pallas import tpu as pltpu
from jax.sharding import PartitionSpec as P

F32, BF16 = jnp.float32, jnp.bfloat16
MIB = 2**20
ANY = pl.BlockSpec(memory_space=pl.ANY)
NT = (((1,), (1,)), ((), ()))
NN = (((1,), (0,)), ((), ()))
TN = (((0,), (0,)), ((), ()))
PARTS = 2
SUB = 4
TILE = 256


def dot(a, b, dims):
    return lax.dot_general(a, b, dims, preferred_element_type=F32)


def ring_kernel(n, x, dy, gate, up, w_gate, w_up, w_down,
                dx, last_0, last_1, dw_gate, dw_up, dw_down,
                wd_v, wc_v, dy_v, g_v, u_v, ht_v, dc_v, buf, ag, x_v, xt_v, dw_v, dd_v,
                wd_sem, wc_sem, in_sem, send_sem, recv_sem, gsend_sem, grecv_sem, end_sem, keep_sem,
                x_sem, dw_sem, dd_sem):
    me = lax.axis_index("tp")
    piece, width, ff = buf.shape[4], buf.shape[5], g_v.shape[-1]
    half = PARTS * piece
    chunks, messages, tiles = n * PARTS, PARTS * SUB, x.shape[1] // TILE

    def block_row(block, d, h):
        return pl.multiple_of((2 * lax.rem(block + 2 * n, n) + d) * half + h * piece, piece)

    def row_of(k, d):
        return block_row(me + (2 * d - 1) * (k // PARTS + 1), d, lax.rem(k, PARTS))

    def load(k):
        slot = lax.rem(k, 2)
        return [
            pltpu.make_async_copy(src.at[pl.ds(row_of(k, d), piece)], dst.at[slot, pl.ds(d * piece, piece)], in_sem.at[i, slot])
            for i, (src, dst) in enumerate(((dy, dy_v), (gate, g_v), (up, u_v)))
            for d in range(2)
        ]

    def whole(ref, sem):
        return pltpu.make_async_copy(ref, ref, sem)

    def loaded(k):
        slot = lax.rem(k, 2)
        return [whole(ref.at[slot], in_sem.at[i, slot]) for i, ref in enumerate((dy_v, g_v, u_v))]

    def down(f):
        rows = pl.ds(f, min(TILE, ff - f))
        return pltpu.make_async_copy(w_down.at[rows], wd_v.at[rows], wd_sem.at[f // TILE])

    def weight(c):
        rows = pl.ds(pl.multiple_of(c * width, width), width)
        return [
            pltpu.make_async_copy(w_gate.at[rows], wc_v.at[rows, pl.ds(0, ff)], wc_sem.at[c]),
            pltpu.make_async_copy(w_up.at[rows], wc_v.at[rows, pl.ds(ff, ff)], wc_sem.at[c]),
        ]

    def weighted(c):
        return whole(wc_v.at[pl.ds(pl.multiple_of(c * width, width), width)], wc_sem.at[c])

    def to(d):
        return {"device_id": {"tp": lax.rem(me + 1 - 2 * d + n, n)}, "device_id_type": pl.DeviceIdType.MESH}

    def hop(s, h, c, d):
        return pltpu.make_async_remote_copy(
            src_ref=buf.at[s, h, c, d], dst_ref=buf.at[s + 1, h, c, d],
            send_sem=send_sem.at[s], recv_sem=recv_sem.at[s, h, c], **to(d),
        )

    def end(h, c, d):
        cols = pl.ds(pl.multiple_of(c * width, width), width)
        return (last_0, last_1)[d].at[pl.ds(pl.multiple_of(h * piece, piece), piece), cols]

    def spread(r, h, c, d):
        return pltpu.make_async_remote_copy(
            src_ref=buf.at[n - 1, h, c, d] if r == 0 else ag.at[r - 1, h, c, d],
            dst_ref=ag.at[r, h, c, d] if r < n - 3 else end(h, c, d),
            send_sem=gsend_sem.at[r], recv_sem=grecv_sem.at[r, h, c] if r < n - 3 else end_sem.at[d], **to(d),
        )

    def keep(r, h, c, d):
        cols = pl.ds(pl.multiple_of(c * width, width), width)
        return pltpu.make_async_copy(
            buf.at[n - 1, h, c, d] if r == 0 else ag.at[r - 1, h, c, d],
            dx.at[pl.ds(block_row(me + (2 * d - 1) * r, d, h), piece), cols], keep_sem.at[r],
        )

    def load_cols(src, j):
        cols = pl.ds(pl.multiple_of(j * TILE, TILE), TILE)
        slot = lax.rem(j, 2)
        return pltpu.make_async_copy(src.at[:, cols], x_v.at[slot], x_sem.at[slot])

    def save_dd(j):
        cols = pl.ds(pl.multiple_of(j * TILE, TILE), TILE)
        slot = lax.rem(j, 2)
        return pltpu.make_async_copy(dd_v.at[slot], dw_down.at[:, cols], dd_sem.at[slot])

    def save_dw(j):
        rows = pl.ds(pl.multiple_of(j * TILE, TILE), TILE)
        slot = lax.rem(j, 2)
        return [
            pltpu.make_async_copy(dw_v.at[slot, :, pl.ds(0, ff)], dw_gate.at[rows], dw_sem.at[slot]),
            pltpu.make_async_copy(dw_v.at[slot, :, pl.ds(ff, ff)], dw_up.at[rows], dw_sem.at[slot]),
        ]

    def saved_dw(j):
        slot = lax.rem(j, 2)
        return whole(dw_v.at[slot], dw_sem.at[slot])

    def start(copies):
        for copy in copies:
            copy.start()

    def wait(copies):
        for copy in copies:
            copy.wait()

    f_tiles = range(0, ff, TILE)
    now, downs = load(0), [down(f) for f in f_tiles]
    start(now[:2] + downs[:3] + now[2:] + downs[3:])

    barrier = pltpu.get_barrier_semaphore()
    for d in range(2):
        pl.semaphore_signal(barrier, inc=1, **to(d))
    buf[0] = jnp.zeros(buf.shape[1:], BF16)

    def grads(k, first=False):
        slot = lax.rem(k, 2)
        copies = loaded(k)
        wait(copies)

        def rest(f, dh):
            size = min(TILE, ff - f)
            cols = pl.ds(f, size)
            g, u = g_v[slot, :, cols].astype(F32), u_v[slot, :, cols].astype(F32)
            sig = jax.nn.sigmoid(g)
            silu = g * sig
            hidden = (silu * u).astype(BF16).T
            d_gate = (dh * u * (sig * (1.0 + g * (1.0 - sig)))).astype(BF16)
            d_up = (dh * silu).astype(BF16)
            for d in range(2):
                rows, part = pl.ds(row_of(k, d), piece), slice(d * piece, (d + 1) * piece)
                dc_v[rows, cols] = d_gate[part]
                dc_v[rows, pl.ds(ff + f, size)] = d_up[part]
                ht_v[cols, rows] = hidden[:, part]

        dh = None
        for f in f_tiles:
            if first and f == 0:
                wait(downs[:3])
                start(weight(0))
            if first and f == 3 * TILE:
                rest(f - TILE, dh)
                wait(downs[3:])
                start(weight(1))
            before, dh = dh, dot(dy_v[slot], wd_v[pl.ds(f, min(TILE, ff - f)), :], NT)
            if f and not (first and f == 3 * TILE):
                rest(f - TILE, before)
        rest(f_tiles[-1], dh)

        @pl.when(k + 2 < chunks)
        def _():
            start(load(k + 2))

    def term(k, c, first=False):
        s, h = k // PARTS, lax.rem(k, PARTS)
        if first:
            weighted(c).wait()

        @pl.when(s > 0)
        def _():
            whole(buf.at[s, h, c], recv_sem.at[s - 1, h, c]).wait()

        cols = pl.ds(pl.multiple_of(c * width, width), width)
        rows = [dc_v[pl.ds(row_of(k, d), piece), :] for d in range(2)]
        acc = dot(jnp.concatenate(rows, axis=0), wc_v[cols, :], NT)
        for d in range(2):
            own = acc[d * piece:(d + 1) * piece]
            buf[s, h, c, d] = (own + buf[s, h, c, d].astype(F32)).astype(BF16)

        @pl.when(s < n - 1)
        def _():
            for d in range(2):
                hop(s, h, c, d).start()

        @pl.when(s == n - 1)
        def _():
            for d in range(2):
                spread(0, h, c, d).start()
                keep(0, h, c, d).start()

    grads(0, first=True)
    start(weight(2) + weight(3) + load(1))
    pl.semaphore_wait(barrier, 2)

    def term0(c, _):
        term(0, c, first=True)
        return 0

    lax.fori_loop(0, SUB, term0, 0)

    def terms(k):
        def body(c, _):
            term(k, c)
            return 0

        lax.fori_loop(0, SUB, body, 0)

    def chunk(k, _):
        grads(k)

        @pl.when(k < chunks - PARTS)
        def _():
            terms(k)
        return 0

    lax.fori_loop(1, chunks, chunk, 0)
    start([load_cols(dy, 0), load_cols(dy, 1)])

    def last_term(m, _):
        term(chunks - PARTS + m // SUB, lax.rem(m, SUB))
        slot = lax.rem(m, 2)
        load_cols(dy, m).wait()

        @pl.when(m >= 2)
        def _():
            save_dd(m - 2).wait()

        dd_v[slot] = dot(ht_v[...], x_v[slot], NN).astype(BF16)
        save_dd(m).start()

        @pl.when(m + 2 < messages)
        def _():
            load_cols(dy, m + 2).start()
        return 0

    lax.fori_loop(0, messages, last_term, 0)
    start([load_cols(x, 0), load_cols(x, 1)])

    def forward(r, m):
        h, c = m // SUB, lax.rem(m, SUB)
        whole(ag.at[r - 1, h, c], grecv_sem.at[r - 1, h, c]).wait()
        for d in range(2):
            spread(r, h, c, d).start()
            keep(r, h, c, d).start()

    per = -(-messages * (n - 3) // tiles)

    def tile(j, _):
        slot = lax.rem(j, 2)
        load_cols(x, j).wait()
        xt_v[...] = x_v[slot].T

        @pl.when(j >= 2)
        def _():
            saved_dw(j - 2).wait()

        for f in range(0, 2 * ff, 2 * TILE):
            cols = pl.ds(f, min(2 * TILE, 2 * ff - f))
            dw_v[slot, :, cols] = dot(xt_v[...], dc_v[:, cols], NN).astype(BF16)
        start(save_dw(j))

        @pl.when(j + 2 < tiles)
        def _():
            load_cols(x, j + 2).start()

        for r in range(1, n - 2):
            for i in range(per):
                m = j * per + i

                @pl.when(m < messages)
                def _():
                    forward(r, m)
        return 0

    lax.fori_loop(0, tiles, tile, 0)

    for s in range(n - 1):
        whole(buf.at[s], send_sem.at[s]).wait()
    for r in range(n - 2):
        sent = buf.at[n - 1] if r == 0 else ag.at[r - 1]
        whole(sent, keep_sem.at[r]).wait()
        whole(sent, gsend_sem.at[r]).wait()
    for j in range(tiles - 2, tiles):
        save_dd(j).wait()
        saved_dw(j).wait()
    for d, ref in enumerate((last_0, last_1)):
        whole(ref, end_sem.at[d]).wait()


def ring(n, x, dy, gate, up, w_gate, w_up, w_down):
    (rows, d), ff = dy.shape, gate.shape[1]
    piece, width = rows // (2 * n * PARTS), d // SUB
    assert n == 4 and d == PARTS * SUB * TILE
    dma = pltpu.SemaphoreType.DMA
    each = (PARTS, SUB, 2)
    return pl.pallas_call(
        functools.partial(ring_kernel, n),
        out_shape=[
            jax.ShapeDtypeStruct((rows, d), BF16),
            jax.ShapeDtypeStruct((PARTS * piece, d), BF16),
            jax.ShapeDtypeStruct((PARTS * piece, d), BF16),
            jax.ShapeDtypeStruct((d, ff), BF16),
            jax.ShapeDtypeStruct((d, ff), BF16),
            jax.ShapeDtypeStruct((ff, d), BF16),
        ],
        in_specs=[ANY] * 7,
        out_specs=[ANY] * 6,
        scratch_shapes=[
            pltpu.VMEM((ff, d), BF16),
            pltpu.VMEM((d, 2 * ff), BF16),
            pltpu.VMEM((2, 2 * piece, d), BF16),
            pltpu.VMEM((2, 2 * piece, ff), BF16),
            pltpu.VMEM((2, 2 * piece, ff), BF16),
            pltpu.VMEM((ff, rows), BF16),
            pltpu.VMEM((rows, 2 * ff), BF16),
            pltpu.VMEM((n, *each, piece, width), BF16),
            pltpu.VMEM((n - 3, *each, piece, width), BF16),
            pltpu.VMEM((2, rows, TILE), BF16),
            pltpu.VMEM((TILE, rows), BF16),
            pltpu.VMEM((2, TILE, 2 * ff), BF16),
            pltpu.VMEM((2, ff, TILE), BF16),
            dma((-(-ff // TILE),)),
            dma((SUB,)),
            dma((3, 2)),
            dma((n - 1,)),
            dma((n - 1, PARTS, SUB)),
            dma((n - 2,)),
            dma((n - 3, PARTS, SUB)),
            dma((2,)),
            dma((n - 2,)),
            dma((2,)),
            dma((2,)),
            dma((2,)),
        ],
        compiler_params=pltpu.CompilerParams(
            collective_id=0, has_side_effects=True, vmem_limit_bytes=62 * MIB
        ),
        cost_estimate=pl.CostEstimate(flops=12 * rows * d * ff, bytes_accessed=16 * rows * d, transcendentals=2 * rows * ff),
        name="ring",
    )(x, dy, gate, up, w_gate, w_up, w_down)


def finish_kernel(count, places, *refs):
    del places
    j, outs = pl.program_id(0), refs[-4:]
    dx_in, last_0, last_1 = refs[:3]
    for src, dst in zip(refs[3:6], outs[1:]):
        dst[...] = src[...]
    for low, high, src in ((0, count, dx_in), (count, count + PARTS, last_0), (count + PARTS, count + 2 * PARTS, last_1)):
        @pl.when((j >= low) & (j < high))
        def _():
            outs[0][...] = src[...]


def finish(n, dx, last_0, last_1, dw_gate, dw_up, dw_down):
    (rows, d), (ff, _) = dx.shape, dw_down.shape
    piece = rows // (2 * n * PARTS)
    count = 2 * (n - 2) * PARTS
    me, i = lax.axis_index("tp"), jnp.arange(count + 2 * PARTS)
    way = i // PARTS % 2
    places = (2 * ((me + (2 * way - 1) * (i // (2 * PARTS)) + n) % n) + way) * PARTS + i % PARTS
    steps = d // 128

    def rows_in(block, most, first=0):
        return pl.BlockSpec(block, lambda j, p: (jnp.clip(j - first, 0, most - 1), 0))

    def placed(most):
        return pl.BlockSpec((piece, d), lambda j, p: (p[jnp.minimum(j, most - 1)], 0))

    weights = [rows_in((128, ff), steps), rows_in((128, ff), steps), rows_in((128, d), ff // 128)]
    return pl.pallas_call(
        functools.partial(finish_kernel, count),
        out_shape=[jax.ShapeDtypeStruct(a.shape, a.dtype) for a in (dx, dw_gate, dw_up, dw_down)],
        grid_spec=pltpu.PrefetchScalarGridSpec(
            num_scalar_prefetch=1,
            grid=(steps,),
            in_specs=[placed(count), rows_in((piece, d), PARTS, count), rows_in((piece, d), PARTS, count + PARTS), *weights],
            out_specs=[placed(count + 2 * PARTS), *weights],
        ),
        compiler_params=pltpu.CompilerParams(vmem_limit_bytes=61 * MIB),
        cost_estimate=pl.CostEstimate(flops=2 * rows * d * ff, bytes_accessed=12 * rows * d, transcendentals=0),
        name="finish",
    )(places, dx, last_0, last_1, dw_gate, dw_up, dw_down)


def place_kernel(n, _, end_0, end_1, dx, sem):
    me, half = lax.axis_index("tp"), end_0.shape[0]
    put = []
    for d, src in enumerate((end_0, end_1)):
        row = (2 * lax.rem(me + (2 * d - 1) * (n - 1) + n, n) + d) * half
        for i in range(4):
            part = half // 4
            rows = pl.ds(pl.multiple_of(row + i * part, part), part)
            put.append(pltpu.make_async_copy(src.at[pl.ds(i * part, part)], dx.at[rows], sem.at[d, i]))
    for copy in put:
        copy.start()
    for copy in put:
        copy.wait()


def place(n, dx, ends):
    vmem = pl.BlockSpec(memory_space=pltpu.VMEM)
    return pl.pallas_call(
        functools.partial(place_kernel, n),
        out_shape=jax.ShapeDtypeStruct(dx.shape, dx.dtype),
        in_specs=[ANY, vmem, vmem],
        out_specs=ANY,
        scratch_shapes=[pltpu.SemaphoreType.DMA((2, 4))],
        input_output_aliases={0: 0},
        compiler_params=pltpu.CompilerParams(vmem_limit_bytes=16 * MIB),
        name="place",
    )(dx, *ends)


def solution(mesh):
    n = mesh.shape["tp"]

    def step(x, dy, gate, up, w_gate, w_up, w_down):
        dx, *last, dw_gate, dw_up, dw_down = ring(n, x, dy, gate, up, w_gate, w_up, w_down)
        ends = [lax.ppermute(last[d], "tp", [(i, (i + 1 - 2 * d) % n) for i in range(n)]) for d in range(2)]
        dx, dw_gate, dw_up, dw_down = finish(n, dx, *last, dw_gate, dw_up, dw_down)
        return place(n, dx, ends), dw_gate, dw_up, dw_down

    tokens, columns, rows = P("dp", None), P(None, "tp"), P("tp", None)
    return jax.shard_map(
        step,
        mesh=mesh,
        in_specs=(tokens, tokens, P("dp", "tp"), P("dp", "tp"), columns, columns, rows),
        out_specs=(tokens, P("dp", "tp"), P("dp", "tp"), P(("dp", "tp"), None)),
        check_vma=False,
    )
```

```python
import functools

import jax
import jax.numpy as jnp
from jax import lax
from jax.experimental import pallas as pl
from jax.experimental.pallas import tpu as pltpu
from jax.sharding import PartitionSpec as P

F32, BF16 = jnp.float32, jnp.bfloat16
MIB = 2**20
ANY = pl.BlockSpec(memory_space=pl.ANY)
NT = (((1,), (1,)), ((), ()))
NN = (((1,), (0,)), ((), ()))
TN = (((0,), (0,)), ((), ()))
PARTS = 2
SUB = 4
TILE = 256
WIDE = 512


def dot(a, b, dims):
    return lax.dot_general(a, b, dims, preferred_element_type=F32)


def ring_kernel(n, x, dy, gate, up, w_gate, w_up, w_down,
                dx, last_0, last_1, dw_gate, dw_up, dw_down,
                wd_v, wc_v, dy_v, g_v, u_v, f_v, ht_v, dc_v, buf, ag, x_v, xt_v, dw_v, dd_v,
                wd_sem, wc_sem, in_sem, send_sem, recv_sem, gsend_sem, grecv_sem, end_sem, keep_sem,
                x_sem, dw_sem, dd_sem):
    me = lax.axis_index("tp")
    piece, width, ff = buf.shape[4], buf.shape[5], g_v.shape[-1]
    half = PARTS * piece
    chunks, messages, tiles = n * PARTS, PARTS * SUB, x.shape[1] // TILE

    def block_row(block, d, h):
        return pl.multiple_of((2 * lax.rem(block + 2 * n, n) + d) * half + h * piece, piece)

    def row_of(k, d):
        return block_row(me + (2 * d - 1) * (k // PARTS + 1), d, lax.rem(k, PARTS))

    def load(k):
        slot = lax.rem(k, 2)
        return [
            pltpu.make_async_copy(src.at[pl.ds(row_of(k, d), piece)], dst.at[slot, pl.ds(d * piece, piece)], in_sem.at[i, slot])
            for i, (src, dst) in enumerate(((dy, dy_v), (gate, g_v), (up, u_v)))
            for d in range(2)
        ]

    def whole(ref, sem):
        return pltpu.make_async_copy(ref, ref, sem)

    def loaded(k):
        slot = lax.rem(k, 2)
        return [whole(ref.at[slot], in_sem.at[i, slot]) for i, ref in enumerate((dy_v, g_v, u_v))]

    def down(f):
        rows = pl.ds(f, min(WIDE, ff - f))
        return pltpu.make_async_copy(w_down.at[rows], wd_v.at[rows], wd_sem.at[f // WIDE])

    def weight(c):
        rows = pl.ds(pl.multiple_of(c * width, width), width)
        return [
            pltpu.make_async_copy(w_gate.at[rows], wc_v.at[rows, pl.ds(0, ff)], wc_sem.at[c]),
            pltpu.make_async_copy(w_up.at[rows], wc_v.at[rows, pl.ds(ff, ff)], wc_sem.at[c]),
        ]

    def weighted(c):
        return whole(wc_v.at[pl.ds(pl.multiple_of(c * width, width), width)], wc_sem.at[c])

    def to(d):
        return {"device_id": {"tp": lax.rem(me + 1 - 2 * d + n, n)}, "device_id_type": pl.DeviceIdType.MESH}

    def hop(s, h, c, d):
        return pltpu.make_async_remote_copy(
            src_ref=buf.at[s, h, c, d], dst_ref=buf.at[s + 1, h, c, d],
            send_sem=send_sem.at[s], recv_sem=recv_sem.at[s, h, c], **to(d),
        )

    def end(h, c, d):
        cols = pl.ds(pl.multiple_of(c * width, width), width)
        return (last_0, last_1)[d].at[pl.ds(pl.multiple_of(h * piece, piece), piece), cols]

    def spread(r, h, c, d):
        return pltpu.make_async_remote_copy(
            src_ref=buf.at[n - 1, h, c, d] if r == 0 else ag.at[r - 1, h, c, d],
            dst_ref=ag.at[r, h, c, d] if r < n - 3 else end(h, c, d),
            send_sem=gsend_sem.at[r], recv_sem=grecv_sem.at[r, h, c] if r < n - 3 else end_sem.at[d], **to(d),
        )

    def keep(r, h, c, d):
        cols = pl.ds(pl.multiple_of(c * width, width), width)
        return pltpu.make_async_copy(
            buf.at[n - 1, h, c, d] if r == 0 else ag.at[r - 1, h, c, d],
            dx.at[pl.ds(block_row(me + (2 * d - 1) * r, d, h), piece), cols], keep_sem.at[r],
        )

    def load_cols(src, j):
        cols = pl.ds(pl.multiple_of(j * TILE, TILE), TILE)
        slot = lax.rem(j, 2)
        return pltpu.make_async_copy(src.at[:, cols], x_v.at[slot], x_sem.at[slot])

    def save_dd(j):
        cols = pl.ds(pl.multiple_of(j * TILE, TILE), TILE)
        slot = lax.rem(j, 2)
        return pltpu.make_async_copy(dd_v.at[slot], dw_down.at[:, cols], dd_sem.at[slot])

    def save_dw(j):
        rows = pl.ds(pl.multiple_of(j * TILE, TILE), TILE)
        slot = lax.rem(j, 2)
        return [
            pltpu.make_async_copy(dw_v.at[slot, :, pl.ds(0, ff)], dw_gate.at[rows], dw_sem.at[slot]),
            pltpu.make_async_copy(dw_v.at[slot, :, pl.ds(ff, ff)], dw_up.at[rows], dw_sem.at[slot]),
        ]

    def saved_dw(j):
        slot = lax.rem(j, 2)
        return whole(dw_v.at[slot], dw_sem.at[slot])

    def start(copies):
        for copy in copies:
            copy.start()

    def wait(copies):
        for copy in copies:
            copy.wait()

    f_tiles = range(0, ff, WIDE)
    now, downs = load(0), [down(f) for f in f_tiles]
    start(now[2:] + now[:2] + downs)

    barrier = pltpu.get_barrier_semaphore()
    for d in range(2):
        pl.semaphore_signal(barrier, inc=1, **to(d))
    buf[0] = jnp.zeros(buf.shape[1:], BF16)

    def span(f):
        return pl.ds(f, min(WIDE, ff - f))

    def factors(slot, cols):
        g, u = g_v[slot, :, cols].astype(F32), u_v[slot, :, cols].astype(F32)
        sig = jax.nn.sigmoid(g)
        return sig * (1.0 + g * (1.0 - sig)), g * sig, u

    def store_grads(k, f, d_gate, d_up):
        for d in range(2):
            rows, part = pl.ds(row_of(k, d), piece), slice(d * piece, (d + 1) * piece)
            dc_v[rows, span(f)] = d_gate[part].astype(BF16)
            dc_v[rows, pl.ds(ff + f, min(WIDE, ff - f))] = d_up[part].astype(BF16)

    def store_hidden(k, f, hidden):
        hidden = hidden.astype(BF16).T
        for d in range(2):
            ht_v[span(f), pl.ds(row_of(k, d), piece)] = hidden[:, d * piece:(d + 1) * piece]

    def first_grads():
        copies = loaded(0)
        wait(copies[1:])
        start(weight(0))
        for f in f_tiles:
            slope, silu, u = factors(0, span(f))
            f_v[0, :, span(f)] = u * slope
            f_v[1, :, span(f)] = silu
        wait(copies[:1])
        for f, copy in zip(f_tiles, downs):
            copy.wait()
            dh = dot(dy_v[0], wd_v[span(f), :], NT)
            store_grads(0, f, dh * f_v[0, :, span(f)], dh * f_v[1, :, span(f)])

    def first_hidden():
        for f in f_tiles:
            _, silu, u = factors(0, span(f))
            store_hidden(0, f, silu * u)
        start(load(2))

    def grads(k):
        slot = lax.rem(k, 2)
        wait(loaded(k))

        def rest(f, dh):
            slope, silu, u = factors(slot, span(f))
            store_hidden(k, f, silu * u)
            store_grads(k, f, dh * u * slope, dh * silu)

        dh = None
        for f in f_tiles:
            before, dh = dh, dot(dy_v[slot], wd_v[span(f), :], NT)
            if f:
                rest(f - WIDE, before)
        rest(f_tiles[-1], dh)

        @pl.when(k + 2 < chunks)
        def _():
            start(load(k + 2))

    def term(k, c, first=False):
        s, h = k // PARTS, lax.rem(k, PARTS)
        if first:
            weighted(c).wait()

        @pl.when(s > 0)
        def _():
            whole(buf.at[s, h, c], recv_sem.at[s - 1, h, c]).wait()

        cols = pl.ds(pl.multiple_of(c * width, width), width)
        rows = [dc_v[pl.ds(row_of(k, d), piece), :] for d in range(2)]
        acc = dot(jnp.concatenate(rows, axis=0), wc_v[cols, :], NT)
        for d in range(2):
            own = acc[d * piece:(d + 1) * piece]
            buf[s, h, c, d] = (own + buf[s, h, c, d].astype(F32)).astype(BF16)

        @pl.when(s < n - 1)
        def _():
            for d in range(2):
                hop(s, h, c, d).start()

        @pl.when(s == n - 1)
        def _():
            for d in range(2):
                spread(0, h, c, d).start()
                keep(0, h, c, d).start()

    first_grads()
    start(weight(1))
    pl.semaphore_wait(barrier, 2)
    term(0, 0, first=True)
    start(weight(2) + weight(3) + load(1))

    def term0(c, _):
        term(0, c, first=True)
        return 0

    lax.fori_loop(1, SUB, term0, 0)
    first_hidden()

    def terms(k):
        def body(c, _):
            term(k, c)
            return 0

        lax.fori_loop(0, SUB, body, 0)

    def chunk(k, _):
        grads(k)

        @pl.when(k < chunks - PARTS)
        def _():
            terms(k)
        return 0

    lax.fori_loop(1, chunks, chunk, 0)
    start([load_cols(dy, 0), load_cols(dy, 1)])

    def last_term(m, _):
        term(chunks - PARTS + m // SUB, lax.rem(m, SUB))
        slot = lax.rem(m, 2)
        load_cols(dy, m).wait()

        @pl.when(m >= 2)
        def _():
            save_dd(m - 2).wait()

        dd_v[slot] = dot(ht_v[...], x_v[slot], NN).astype(BF16)
        save_dd(m).start()

        @pl.when(m + 2 < messages)
        def _():
            load_cols(dy, m + 2).start()
        return 0

    lax.fori_loop(0, messages, last_term, 0)
    start([load_cols(x, 0), load_cols(x, 1)])

    def forward(r, m):
        h, c = m // SUB, lax.rem(m, SUB)
        whole(ag.at[r - 1, h, c], grecv_sem.at[r - 1, h, c]).wait()
        for d in range(2):
            spread(r, h, c, d).start()
            keep(r, h, c, d).start()

    per = -(-messages * (n - 3) // tiles)

    def tile(j, _):
        slot = lax.rem(j, 2)
        load_cols(x, j).wait()
        xt_v[...] = x_v[slot].T

        @pl.when(j >= 2)
        def _():
            saved_dw(j - 2).wait()

        for f in range(0, 2 * ff, 2 * TILE):
            cols = pl.ds(f, min(2 * TILE, 2 * ff - f))
            dw_v[slot, :, cols] = dot(xt_v[...], dc_v[:, cols], NN).astype(BF16)
        start(save_dw(j))

        @pl.when(j + 2 < tiles)
        def _():
            load_cols(x, j + 2).start()

        for r in range(1, n - 2):
            for i in range(per):
                m = j * per + i

                @pl.when(m < messages)
                def _():
                    forward(r, m)
        return 0

    lax.fori_loop(0, tiles, tile, 0)

    for s in range(n - 1):
        whole(buf.at[s], send_sem.at[s]).wait()
    for r in range(n - 2):
        sent = buf.at[n - 1] if r == 0 else ag.at[r - 1]
        whole(sent, keep_sem.at[r]).wait()
        whole(sent, gsend_sem.at[r]).wait()
    for j in range(tiles - 2, tiles):
        save_dd(j).wait()
        saved_dw(j).wait()
    for d, ref in enumerate((last_0, last_1)):
        whole(ref, end_sem.at[d]).wait()


def ring(n, x, dy, gate, up, w_gate, w_up, w_down):
    (rows, d), ff = dy.shape, gate.shape[1]
    piece, width = rows // (2 * n * PARTS), d // SUB
    assert n == 4 and d == PARTS * SUB * TILE
    dma = pltpu.SemaphoreType.DMA
    each = (PARTS, SUB, 2)
    return pl.pallas_call(
        functools.partial(ring_kernel, n),
        out_shape=[
            jax.ShapeDtypeStruct((rows, d), BF16),
            jax.ShapeDtypeStruct((PARTS * piece, d), BF16),
            jax.ShapeDtypeStruct((PARTS * piece, d), BF16),
            jax.ShapeDtypeStruct((d, ff), BF16),
            jax.ShapeDtypeStruct((d, ff), BF16),
            jax.ShapeDtypeStruct((ff, d), BF16),
        ],
        in_specs=[ANY] * 7,
        out_specs=[ANY] * 6,
        scratch_shapes=[
            pltpu.VMEM((ff, d), BF16),
            pltpu.VMEM((d, 2 * ff), BF16),
            pltpu.VMEM((2, 2 * piece, d), BF16),
            pltpu.VMEM((2, 2 * piece, ff), BF16),
            pltpu.VMEM((2, 2 * piece, ff), BF16),
            pltpu.VMEM((2, 2 * piece, ff), F32),
            pltpu.VMEM((ff, rows), BF16),
            pltpu.VMEM((rows, 2 * ff), BF16),
            pltpu.VMEM((n, *each, piece, width), BF16),
            pltpu.VMEM((n - 3, *each, piece, width), BF16),
            pltpu.VMEM((2, rows, TILE), BF16),
            pltpu.VMEM((TILE, rows), BF16),
            pltpu.VMEM((2, TILE, 2 * ff), BF16),
            pltpu.VMEM((2, ff, TILE), BF16),
            dma((-(-ff // WIDE),)),
            dma((SUB,)),
            dma((3, 2)),
            dma((n - 1,)),
            dma((n - 1, PARTS, SUB)),
            dma((n - 2,)),
            dma((n - 3, PARTS, SUB)),
            dma((2,)),
            dma((n - 2,)),
            dma((2,)),
            dma((2,)),
            dma((2,)),
        ],
        compiler_params=pltpu.CompilerParams(
            collective_id=0, has_side_effects=True, vmem_limit_bytes=62 * MIB
        ),
        cost_estimate=pl.CostEstimate(flops=12 * rows * d * ff, bytes_accessed=16 * rows * d, transcendentals=2 * rows * ff),
        name="ring",
    )(x, dy, gate, up, w_gate, w_up, w_down)


def finish_kernel(count, places, *refs):
    del places
    j, outs = pl.program_id(0), refs[-4:]
    dx_in, last_0, last_1 = refs[:3]
    for src, dst in zip(refs[3:6], outs[1:]):
        dst[...] = src[...]
    for low, high, src in ((0, count, dx_in), (count, count + PARTS, last_0), (count + PARTS, count + 2 * PARTS, last_1)):
        @pl.when((j >= low) & (j < high))
        def _():
            outs[0][...] = src[...]


def finish(n, dx, last_0, last_1, dw_gate, dw_up, dw_down):
    (rows, d), (ff, _) = dx.shape, dw_down.shape
    piece = rows // (2 * n * PARTS)
    count = 2 * (n - 2) * PARTS
    me, i = lax.axis_index("tp"), jnp.arange(count + 2 * PARTS)
    way = i // PARTS % 2
    places = (2 * ((me + (2 * way - 1) * (i // (2 * PARTS)) + n) % n) + way) * PARTS + i % PARTS
    steps = d // 128

    def rows_in(block, most, first=0):
        return pl.BlockSpec(block, lambda j, p: (jnp.clip(j - first, 0, most - 1), 0))

    def placed(most):
        return pl.BlockSpec((piece, d), lambda j, p: (p[jnp.minimum(j, most - 1)], 0))

    weights = [rows_in((128, ff), steps), rows_in((128, ff), steps), rows_in((128, d), ff // 128)]
    return pl.pallas_call(
        functools.partial(finish_kernel, count),
        out_shape=[jax.ShapeDtypeStruct(a.shape, a.dtype) for a in (dx, dw_gate, dw_up, dw_down)],
        grid_spec=pltpu.PrefetchScalarGridSpec(
            num_scalar_prefetch=1,
            grid=(steps,),
            in_specs=[placed(count), rows_in((piece, d), PARTS, count), rows_in((piece, d), PARTS, count + PARTS), *weights],
            out_specs=[placed(count + 2 * PARTS), *weights],
        ),
        compiler_params=pltpu.CompilerParams(vmem_limit_bytes=61 * MIB),
        cost_estimate=pl.CostEstimate(flops=2 * rows * d * ff, bytes_accessed=12 * rows * d, transcendentals=0),
        name="finish",
    )(places, dx, last_0, last_1, dw_gate, dw_up, dw_down)


def place_kernel(n, _, end_0, end_1, dx, sem):
    me, half = lax.axis_index("tp"), end_0.shape[0]
    put = []
    for d, src in enumerate((end_0, end_1)):
        row = (2 * lax.rem(me + (2 * d - 1) * (n - 1) + n, n) + d) * half
        for i in range(4):
            part = half // 4
            rows = pl.ds(pl.multiple_of(row + i * part, part), part)
            put.append(pltpu.make_async_copy(src.at[pl.ds(i * part, part)], dx.at[rows], sem.at[d, i]))
    for copy in put:
        copy.start()
    for copy in put:
        copy.wait()


def place(n, dx, ends):
    vmem = pl.BlockSpec(memory_space=pltpu.VMEM)
    return pl.pallas_call(
        functools.partial(place_kernel, n),
        out_shape=jax.ShapeDtypeStruct(dx.shape, dx.dtype),
        in_specs=[ANY, vmem, vmem],
        out_specs=ANY,
        scratch_shapes=[pltpu.SemaphoreType.DMA((2, 4))],
        input_output_aliases={0: 0},
        compiler_params=pltpu.CompilerParams(vmem_limit_bytes=16 * MIB),
        name="place",
    )(dx, *ends)


def solution(mesh):
    n = mesh.shape["tp"]

    def step(x, dy, gate, up, w_gate, w_up, w_down):
        dx, *last, dw_gate, dw_up, dw_down = ring(n, x, dy, gate, up, w_gate, w_up, w_down)
        ends = [lax.ppermute(last[d], "tp", [(i, (i + 1 - 2 * d) % n) for i in range(n)]) for d in range(2)]
        dx, dw_gate, dw_up, dw_down = finish(n, dx, *last, dw_gate, dw_up, dw_down)
        return place(n, dx, ends), dw_gate, dw_up, dw_down

    tokens, columns, rows = P("dp", None), P(None, "tp"), P("tp", None)
    return jax.shard_map(
        step,
        mesh=mesh,
        in_specs=(tokens, tokens, P("dp", "tp"), P("dp", "tp"), columns, columns, rows),
        out_specs=(tokens, P("dp", "tp"), P("dp", "tp"), P(("dp", "tp"), None)),
        check_vma=False,
    )
```

```python
import functools

import jax
import jax.numpy as jnp
from jax import lax
from jax.experimental import pallas as pl
from jax.experimental.pallas import tpu as pltpu
from jax.sharding import PartitionSpec as P

F32, BF16 = jnp.float32, jnp.bfloat16
MIB = 2**20
ANY = pl.BlockSpec(memory_space=pl.ANY)
NT = (((1,), (1,)), ((), ()))
NN = (((1,), (0,)), ((), ()))
TN = (((0,), (0,)), ((), ()))
COPIES = 4
PARTS = 2
SUB = 4
TILE = 256
WIDE = 512


def dot(a, b, dims):
    return lax.dot_general(a, b, dims, preferred_element_type=F32)


def ring_kernel(n, x, dy, gate, up, w_gate, w_up, w_down,
                dx, last_0, last_1, dw_gate, dw_up, dw_down,
                wd_v, wc_v, dy_v, g_v, u_v, f_v, ht_v, dc_v, buf, ag, x_v, xt_v, dd_v,
                wd_sem, wc_sem, in_sem, send_sem, recv_sem, gsend_sem, grecv_sem, end_sem, keep_sem,
                x_sem, dw_sem, dd_sem):
    me = lax.axis_index("tp")
    piece, width, ff = buf.shape[4], buf.shape[5], g_v.shape[-1]
    half = PARTS * piece
    chunks, messages, tiles = n * PARTS, PARTS * SUB, x.shape[1] // TILE

    def block_row(block, d, h):
        return pl.multiple_of((2 * lax.rem(block + 2 * n, n) + d) * half + h * piece, piece)

    def row_of(k, d):
        return block_row(me + (2 * d - 1) * (k // PARTS + 1), d, lax.rem(k, PARTS))

    def load(k):
        slot = lax.rem(k, 2)
        return [
            pltpu.make_async_copy(src.at[pl.ds(row_of(k, d), piece)], dst.at[slot, pl.ds(d * piece, piece)], in_sem.at[i, slot])
            for i, (src, dst) in enumerate(((dy, dy_v), (gate, g_v), (up, u_v)))
            for d in range(2)
        ]

    def whole(ref, sem):
        return pltpu.make_async_copy(ref, ref, sem)

    def loaded(k):
        slot = lax.rem(k, 2)
        return [whole(ref.at[slot], in_sem.at[i, slot]) for i, ref in enumerate((dy_v, g_v, u_v))]

    def down(f):
        rows = pl.ds(f, min(WIDE, ff - f))
        return pltpu.make_async_copy(w_down.at[rows], wd_v.at[rows], wd_sem.at[f // WIDE])

    def weight(c):
        rows = pl.ds(pl.multiple_of(c * width, width), width)
        return [
            pltpu.make_async_copy(w_gate.at[rows], wc_v.at[rows, pl.ds(0, ff)], wc_sem.at[c]),
            pltpu.make_async_copy(w_up.at[rows], wc_v.at[rows, pl.ds(ff, ff)], wc_sem.at[c]),
        ]

    def weighted(c):
        return whole(wc_v.at[pl.ds(pl.multiple_of(c * width, width), width)], wc_sem.at[c])

    def to(d):
        return {"device_id": {"tp": lax.rem(me + 1 - 2 * d + n, n)}, "device_id_type": pl.DeviceIdType.MESH}

    def hop(s, h, c, d):
        return pltpu.make_async_remote_copy(
            src_ref=buf.at[s, h, c, d], dst_ref=buf.at[s + 1, h, c, d],
            send_sem=send_sem.at[s], recv_sem=recv_sem.at[s, h, c], **to(d),
        )

    def end(h, c, d):
        cols = pl.ds(pl.multiple_of(c * width, width), width)
        return (last_0, last_1)[d].at[pl.ds(pl.multiple_of(h * piece, piece), piece), cols]

    def spread(r, h, c, d):
        return pltpu.make_async_remote_copy(
            src_ref=buf.at[n - 1, h, c, d] if r == 0 else ag.at[r - 1, h, c, d],
            dst_ref=ag.at[r, h, c, d] if r < n - 3 else end(h, c, d),
            send_sem=gsend_sem.at[r], recv_sem=grecv_sem.at[r, h, c] if r < n - 3 else end_sem.at[d], **to(d),
        )

    def keep(r, h, c, d):
        cols = pl.ds(pl.multiple_of(c * width, width), width)
        return pltpu.make_async_copy(
            buf.at[n - 1, h, c, d] if r == 0 else ag.at[r - 1, h, c, d],
            dx.at[pl.ds(block_row(me + (2 * d - 1) * r, d, h), piece), cols], keep_sem.at[r],
        )

    def load_cols(src, j):
        cols = pl.ds(pl.multiple_of(j * TILE, TILE), TILE)
        slot = lax.rem(j, 2)
        return pltpu.make_async_copy(src.at[:, cols], x_v.at[slot], x_sem.at[slot])

    def save_dd(j):
        cols = pl.ds(pl.multiple_of(j * TILE, TILE), TILE)
        slot = lax.rem(j, 2)
        return pltpu.make_async_copy(dd_v.at[slot], dw_down.at[:, cols], dd_sem.at[slot])

    dws = (g_v, dw_gate), (u_v, dw_up)

    def save_dw(j):
        rows = pl.ds(pl.multiple_of(j * TILE, TILE), TILE)
        slot = lax.rem(j, 2)
        return [pltpu.make_async_copy(v.at[slot], out.at[rows], dw_sem.at[i, slot]) for i, (v, out) in enumerate(dws)]

    def start(copies):
        for copy in copies:
            copy.start()

    def wait(copies):
        for copy in copies:
            copy.wait()

    f_tiles = range(0, ff, WIDE)
    now, downs = load(0), [down(f) for f in f_tiles]
    start(now[2:] + now[:2] + downs)

    barrier = pltpu.get_barrier_semaphore()
    for d in range(2):
        pl.semaphore_signal(barrier, inc=1, **to(d))
    buf[0] = jnp.zeros(buf.shape[1:], BF16)

    def span(f):
        return pl.ds(f, min(WIDE, ff - f))

    def factors(slot, cols):
        g, u = g_v[slot, :, cols].astype(F32), u_v[slot, :, cols].astype(F32)
        sig = jax.nn.sigmoid(g)
        return sig * (1.0 + g * (1.0 - sig)), g * sig, u

    def store_grads(k, f, d_gate, d_up):
        for d in range(2):
            rows, part = pl.ds(row_of(k, d), piece), slice(d * piece, (d + 1) * piece)
            dc_v[rows, span(f)] = d_gate[part].astype(BF16)
            dc_v[rows, pl.ds(ff + f, min(WIDE, ff - f))] = d_up[part].astype(BF16)

    def store_hidden(k, f, hidden):
        hidden = hidden.astype(BF16).T
        for d in range(2):
            ht_v[span(f), pl.ds(row_of(k, d), piece)] = hidden[:, d * piece:(d + 1) * piece]

    def first_grads():
        copies = loaded(0)
        wait(copies[1:])
        start(weight(0))
        for f in f_tiles:
            slope, silu, u = factors(0, span(f))
            f_v[0, :, span(f)] = u * slope
            f_v[1, :, span(f)] = silu
        wait(copies[:1])
        for f, copy in zip(f_tiles, downs):
            copy.wait()
            dh = dot(dy_v[0], wd_v[span(f), :], NT)
            store_grads(0, f, dh * f_v[0, :, span(f)], dh * f_v[1, :, span(f)])

    def first_hidden():
        for f in f_tiles:
            _, silu, u = factors(0, span(f))
            store_hidden(0, f, silu * u)
        start(load(2))

    def grads(k):
        slot = lax.rem(k, 2)
        wait(loaded(k))

        def rest(f, dh):
            slope, silu, u = factors(slot, span(f))
            store_hidden(k, f, silu * u)
            store_grads(k, f, dh * u * slope, dh * silu)

        dh = None
        for f in f_tiles:
            before, dh = dh, dot(dy_v[slot], wd_v[span(f), :], NT)
            if f:
                rest(f - WIDE, before)
        rest(f_tiles[-1], dh)

        @pl.when(k + 2 < chunks)
        def _():
            start(load(k + 2))

    def term(k, c, first=False):
        s, h = k // PARTS, lax.rem(k, PARTS)
        if first:
            weighted(c).wait()

        @pl.when(s > 0)
        def _():
            whole(buf.at[s, h, c], recv_sem.at[s - 1, h, c]).wait()

        cols = pl.ds(pl.multiple_of(c * width, width), width)
        rows = [dc_v[pl.ds(row_of(k, d), piece), :] for d in range(2)]
        acc = dot(jnp.concatenate(rows, axis=0), wc_v[cols, :], NT)
        for d in range(2):
            own = acc[d * piece:(d + 1) * piece]
            buf[s, h, c, d] = (own + buf[s, h, c, d].astype(F32)).astype(BF16)

        @pl.when(s < n - 1)
        def _():
            for d in range(2):
                hop(s, h, c, d).start()

        @pl.when(s == n - 1)
        def _():
            for d in range(2):
                spread(0, h, c, d).start()
                keep(0, h, c, d).start()

    first_grads()
    start(weight(1))
    pl.semaphore_wait(barrier, 2)
    term(0, 0, first=True)
    start(weight(2) + weight(3) + load(1))

    def term0(c, _):
        term(0, c, first=True)
        return 0

    lax.fori_loop(1, SUB, term0, 0)
    first_hidden()

    def terms(k):
        def body(c, _):
            term(k, c)
            return 0

        lax.fori_loop(0, SUB, body, 0)

    def chunk(k, _):
        grads(k)

        @pl.when(k < chunks - PARTS)
        def _():
            terms(k)
        return 0

    lax.fori_loop(1, chunks, chunk, 0)
    start([load_cols(dy, 0), load_cols(dy, 1)])

    def last_term(m, _):
        term(chunks - PARTS + m // SUB, lax.rem(m, SUB))
        slot = lax.rem(m, 2)
        load_cols(dy, m).wait()

        @pl.when(m >= 2)
        def _():
            save_dd(m - 2).wait()

        dd_v[slot] = dot(ht_v[...], x_v[slot], NN).astype(BF16)
        save_dd(m).start()

        @pl.when(m + 2 < messages)
        def _():
            load_cols(dy, m + 2).start()
        return 0

    lax.fori_loop(0, messages, last_term, 0)
    start([load_cols(x, 0), load_cols(x, 1)])

    def forward(r, m):
        h, c = m // SUB, lax.rem(m, SUB)
        whole(ag.at[r - 1, h, c], grecv_sem.at[r - 1, h, c]).wait()
        for d in range(2):
            spread(r, h, c, d).start()
            keep(r, h, c, d).start()

    per = -(-messages * (n - 3) // tiles)

    def tile(j, _):
        slot = lax.rem(j, 2)
        load_cols(x, j).wait()
        xt_v[...] = x_v[slot].T

        @pl.when(j >= 2)
        def _():
            wait(save_dw(j - 2))

        for i, (v, _) in enumerate(dws):
            for f in f_tiles:
                v[slot, :, span(f)] = dot(xt_v[...], dc_v[:, pl.ds(i * ff + f, min(WIDE, ff - f))], NN).astype(BF16)
        start(save_dw(j))

        @pl.when(j + 2 < tiles)
        def _():
            load_cols(x, j + 2).start()

        for r in range(1, n - 2):
            for i in range(per):
                m = j * per + i

                @pl.when(m < messages)
                def _():
                    forward(r, m)
        return 0

    lax.fori_loop(0, tiles, tile, 0)

    for s in range(n - 1):
        whole(buf.at[s], send_sem.at[s]).wait()
    for r in range(n - 2):
        sent = buf.at[n - 1] if r == 0 else ag.at[r - 1]
        whole(sent, keep_sem.at[r]).wait()
        whole(sent, gsend_sem.at[r]).wait()
    for j in range(tiles - 2, tiles):
        save_dd(j).wait()
        wait(save_dw(j))
    for d, ref in enumerate((last_0, last_1)):
        whole(ref, end_sem.at[d]).wait()


def ring(n, x, dy, gate, up, w_gate, w_up, w_down):
    (rows, d), ff = dy.shape, gate.shape[1]
    piece, width = rows // (2 * n * PARTS), d // SUB
    assert TILE == 2 * piece
    assert n > 3 and d == PARTS * SUB * TILE
    dma = pltpu.SemaphoreType.DMA
    each = (PARTS, SUB, 2)
    return pl.pallas_call(
        functools.partial(ring_kernel, n),
        out_shape=[
            jax.ShapeDtypeStruct((rows, d), BF16),
            jax.ShapeDtypeStruct((PARTS * piece, d), BF16),
            jax.ShapeDtypeStruct((PARTS * piece, d), BF16),
            jax.ShapeDtypeStruct((d, ff), BF16),
            jax.ShapeDtypeStruct((d, ff), BF16),
            jax.ShapeDtypeStruct((ff, d), BF16),
        ],
        in_specs=[ANY] * 7,
        out_specs=[ANY] * 6,
        scratch_shapes=[
            pltpu.VMEM((ff, d), BF16),
            pltpu.VMEM((d, 2 * ff), BF16),
            pltpu.VMEM((2, 2 * piece, d), BF16),
            pltpu.VMEM((2, 2 * piece, ff), BF16),
            pltpu.VMEM((2, 2 * piece, ff), BF16),
            pltpu.VMEM((2, 2 * piece, ff), F32),
            pltpu.VMEM((ff, rows), BF16),
            pltpu.VMEM((rows, 2 * ff), BF16),
            pltpu.VMEM((n, *each, piece, width), BF16),
            pltpu.VMEM((n - 3, *each, piece, width), BF16),
            pltpu.VMEM((2, rows, TILE), BF16),
            pltpu.VMEM((TILE, rows), BF16),
            pltpu.VMEM((2, ff, TILE), BF16),
            dma((-(-ff // WIDE),)),
            dma((SUB,)),
            dma((3, 2)),
            dma((n - 1,)),
            dma((n - 1, PARTS, SUB)),
            dma((n - 2,)),
            dma((n - 3, PARTS, SUB)),
            dma((2,)),
            dma((n - 2,)),
            dma((2,)),
            dma((2, 2)),
            dma((2,)),
        ],
        compiler_params=pltpu.CompilerParams(
            collective_id=0, has_side_effects=True, vmem_limit_bytes=62 * MIB
        ),
        cost_estimate=pl.CostEstimate(flops=12 * rows * d * ff, bytes_accessed=16 * rows * d, transcendentals=2 * rows * ff),
        name="ring",
    )(x, dy, gate, up, w_gate, w_up, w_down)


def finish_kernel(n, dx_in, last_0, last_1, dw_gate_in, dw_up_in, dw_down_in, dx, dw_gate, dw_up, dw_down,
                  dx_v, dg_v, du_v, dd_v, in_sem, out_sem):
    me, half = lax.axis_index("tp"), last_0.shape[0]
    moves = []
    for i in range(2 * (n - 1)):
        r, d = i // 2, i % 2
        rows = pl.ds(pl.multiple_of((2 * lax.rem(me + (2 * d - 1) * r + n, n) + d) * half, half), half)
        moves.append((dx_in.at[rows] if r < n - 2 else (last_0, last_1)[d], dx_v.at[i], dx.at[rows]))
    for i in range(COPIES):
        for src, v, dst in ((dw_gate_in, dg_v, dw_gate), (dw_up_in, du_v, dw_up), (dw_down_in, dd_v, dw_down)):
            rows = pl.ds(i * (v.shape[0] // COPIES), v.shape[0] // COPIES)
            moves.append((src.at[rows], v.at[rows], dst.at[rows]))
    bring = [pltpu.make_async_copy(a, b, in_sem.at[i]) for i, (a, b, _) in enumerate(moves)]
    put = [pltpu.make_async_copy(b, c, out_sem.at[i]) for i, (_, b, c) in enumerate(moves)]
    for copy in bring:
        copy.start()
    for copy, after in zip(bring, put):
        copy.wait()
        after.start()
    for copy in put:
        copy.wait()


def finish(n, dx, last_0, last_1, dw_gate, dw_up, dw_down):
    (rows, d), (ff, _) = dx.shape, dw_down.shape
    count = 2 * (n - 1) + 3 * COPIES
    dma = pltpu.SemaphoreType.DMA
    return pl.pallas_call(
        functools.partial(finish_kernel, n),
        out_shape=[jax.ShapeDtypeStruct(a.shape, a.dtype) for a in (dx, dw_gate, dw_up, dw_down)],
        in_specs=[ANY] * 6,
        out_specs=[ANY] * 4,
        scratch_shapes=[
            pltpu.VMEM((2 * (n - 1), *last_0.shape), BF16),
            *(pltpu.VMEM(a.shape, BF16) for a in (dw_gate, dw_up, dw_down)),
            dma((count,)),
            dma((count,)),
        ],
        compiler_params=pltpu.CompilerParams(vmem_limit_bytes=61 * MIB),
        cost_estimate=pl.CostEstimate(flops=2 * rows * d * ff, bytes_accessed=12 * rows * d, transcendentals=0),
        name="finish",
    )(dx, last_0, last_1, dw_gate, dw_up, dw_down)


def place_kernel(n, d, _, end, dx, sem):
    me, half = lax.axis_index("tp"), end.shape[0]
    row, part = (2 * lax.rem(me + (2 * d - 1) * (n - 1) + n, n) + d) * half, half // COPIES
    put = [
        pltpu.make_async_copy(
            end.at[pl.ds(i * part, part)], dx.at[pl.ds(pl.multiple_of(row + i * part, part), part)], sem.at[i]
        )
        for i in range(COPIES)
    ]
    for copy in put:
        copy.start()
    for copy in put:
        copy.wait()


def place(n, d, dx, end):
    return pl.pallas_call(
        functools.partial(place_kernel, n, d),
        out_shape=jax.ShapeDtypeStruct(dx.shape, dx.dtype),
        in_specs=[ANY, pl.BlockSpec(memory_space=pltpu.VMEM)],
        out_specs=ANY,
        scratch_shapes=[pltpu.SemaphoreType.DMA((COPIES,))],
        input_output_aliases={0: 0},
        compiler_params=pltpu.CompilerParams(vmem_limit_bytes=16 * MIB),
        name=f"place_{d}",
    )(dx, end)


def solution(mesh):
    n = mesh.shape["tp"]

    def step(x, dy, gate, up, w_gate, w_up, w_down):
        dx, *last, dw_gate, dw_up, dw_down = ring(n, x, dy, gate, up, w_gate, w_up, w_down)
        ends = [lax.ppermute(last[d], "tp", [(i, (i + 1 - 2 * d) % n) for i in range(n)]) for d in range(2)]
        dx, dw_gate, dw_up, dw_down = finish(n, dx, *last, dw_gate, dw_up, dw_down)
        for d in (1, 0):
            dx = place(n, d, dx, ends[d])
        return dx, dw_gate, dw_up, dw_down

    tokens, columns, rows = P("dp", None), P(None, "tp"), P("tp", None)
    return jax.shard_map(
        step,
        mesh=mesh,
        in_specs=(tokens, tokens, P("dp", "tp"), P("dp", "tp"), columns, columns, rows),
        out_specs=(tokens, P("dp", "tp"), P("dp", "tp"), P(("dp", "tp"), None)),
        check_vma=False,
    )
```

```python
import functools

import jax
import jax.numpy as jnp
from jax import lax
from jax.experimental import pallas as pl
from jax.experimental.pallas import tpu as pltpu
from jax.sharding import PartitionSpec as P

F32, BF16 = jnp.float32, jnp.bfloat16
MIB = 2**20
ANY = pl.BlockSpec(memory_space=pl.ANY)
NT = (((1,), (1,)), ((), ()))
NN = (((1,), (0,)), ((), ()))
TN = (((0,), (0,)), ((), ()))
COPIES = 4
PARTS = 2
SUB = 4
TILE = 256
WIDE = 512


def dot(a, b, dims):
    return lax.dot_general(a, b, dims, preferred_element_type=F32)


def ring_kernel(n, x, dy, gate, up, w_gate, w_up, w_down,
                dx, last_0, last_1, dw_gate, dw_up, dw_down,
                wd_v, wc_v, dy_v, g_v, u_v, f_v, ht_v, dc_v, buf, ag, x_v, xt_v, dd_v,
                wd_sem, wc_sem, in_sem, send_sem, recv_sem, gsend_sem, grecv_sem, end_sem, keep_sem,
                x_sem, dw_sem, dd_sem):
    me = lax.axis_index("tp")
    piece, width, ff = buf.shape[4], buf.shape[5], g_v.shape[-1]
    half = PARTS * piece
    chunks, messages, tiles = n * PARTS, PARTS * SUB, x.shape[1] // TILE

    def block_row(block, d, h):
        return pl.multiple_of((2 * lax.rem(block + 2 * n, n) + d) * half + h * piece, piece)

    def row_of(k, d):
        return block_row(me + (2 * d - 1) * (k // PARTS + 1), d, lax.rem(k, PARTS))

    def load(k):
        slot = lax.rem(k, 2)
        return [
            pltpu.make_async_copy(src.at[pl.ds(row_of(k, d), piece)], dst.at[slot, pl.ds(d * piece, piece)], in_sem.at[i, slot])
            for i, (src, dst) in enumerate(((dy, dy_v), (gate, g_v), (up, u_v)))
            for d in range(2)
        ]

    def whole(ref, sem):
        return pltpu.make_async_copy(ref, ref, sem)

    def loaded(k):
        slot = lax.rem(k, 2)
        return [whole(ref.at[slot], in_sem.at[i, slot]) for i, ref in enumerate((dy_v, g_v, u_v))]

    def down(f):
        rows = pl.ds(f, min(WIDE, ff - f))
        return pltpu.make_async_copy(w_down.at[rows], wd_v.at[rows], wd_sem.at[f // WIDE])

    def weight(c):
        rows = pl.ds(pl.multiple_of(c * width, width), width)
        return [
            pltpu.make_async_copy(w_gate.at[rows], wc_v.at[rows, pl.ds(0, ff)], wc_sem.at[c]),
            pltpu.make_async_copy(w_up.at[rows], wc_v.at[rows, pl.ds(ff, ff)], wc_sem.at[c]),
        ]

    def weighted(c):
        return whole(wc_v.at[pl.ds(pl.multiple_of(c * width, width), width)], wc_sem.at[c])

    def to(d):
        return {"device_id": {"tp": lax.rem(me + 1 - 2 * d + n, n)}, "device_id_type": pl.DeviceIdType.MESH}

    def hop(s, h, c, d):
        return pltpu.make_async_remote_copy(
            src_ref=buf.at[s, h, c, d], dst_ref=buf.at[s + 1, h, c, d],
            send_sem=send_sem, recv_sem=recv_sem.at[s, h, c], **to(d),
        )

    def end(h, c, d):
        cols = pl.ds(pl.multiple_of(c * width, width), width)
        return (last_0, last_1)[d].at[pl.ds(pl.multiple_of(h * piece, piece), piece), cols]

    def spread(r, h, c, d):
        return pltpu.make_async_remote_copy(
            src_ref=buf.at[n - 1, h, c, d] if r == 0 else ag.at[r - 1, h, c, d],
            dst_ref=ag.at[r, h, c, d] if r < n - 3 else end(h, c, d),
            send_sem=gsend_sem.at[r], recv_sem=grecv_sem.at[r, h, c] if r < n - 3 else end_sem.at[d], **to(d),
        )

    def keep(r, h, c, d):
        cols = pl.ds(pl.multiple_of(c * width, width), width)
        return pltpu.make_async_copy(
            buf.at[n - 1, h, c, d] if r == 0 else ag.at[r - 1, h, c, d],
            dx.at[pl.ds(block_row(me + (2 * d - 1) * r, d, h), piece), cols], keep_sem.at[r],
        )

    def load_cols(src, j):
        cols = pl.ds(pl.multiple_of(j * TILE, TILE), TILE)
        slot = lax.rem(j, 2)
        return pltpu.make_async_copy(src.at[:, cols], x_v.at[slot], x_sem.at[slot])

    def save_dd(j):
        cols = pl.ds(pl.multiple_of(j * TILE, TILE), TILE)
        slot = lax.rem(j, 2)
        return pltpu.make_async_copy(dd_v.at[slot], dw_down.at[:, cols], dd_sem.at[slot])

    dws = (g_v, dw_gate), (u_v, dw_up)

    def save_dw(j):
        rows = pl.ds(pl.multiple_of(j * TILE, TILE), TILE)
        slot = lax.rem(j, 2)
        return [pltpu.make_async_copy(v.at[slot], out.at[rows], dw_sem.at[i, slot]) for i, (v, out) in enumerate(dws)]

    def start(copies):
        for copy in copies:
            copy.start()

    def wait(copies):
        for copy in copies:
            copy.wait()

    f_tiles = range(0, ff, WIDE)
    now, downs = load(0), [down(f) for f in f_tiles]
    start(now[2:] + now[:2] + downs)

    barrier = pltpu.get_barrier_semaphore()
    for d in range(2):
        pl.semaphore_signal(barrier, inc=1, **to(d))
    buf[0] = jnp.zeros(buf.shape[1:], BF16)

    def span(f):
        return pl.ds(f, min(WIDE, ff - f))

    def factors(slot, cols):
        g, u = g_v[slot, :, cols].astype(F32), u_v[slot, :, cols].astype(F32)
        sig = jax.nn.sigmoid(g)
        return sig * (1.0 + g * (1.0 - sig)), g * sig, u

    def store_grads(k, f, d_gate, d_up):
        for d in range(2):
            rows, part = pl.ds(row_of(k, d), piece), slice(d * piece, (d + 1) * piece)
            dc_v[rows, span(f)] = d_gate[part].astype(BF16)
            dc_v[rows, pl.ds(ff + f, min(WIDE, ff - f))] = d_up[part].astype(BF16)

    def store_hidden(k, f, hidden):
        hidden = hidden.astype(BF16).T
        for d in range(2):
            ht_v[span(f), pl.ds(row_of(k, d), piece)] = hidden[:, d * piece:(d + 1) * piece]

    def first_grads():
        copies = loaded(0)
        wait(copies[1:])
        start(weight(0))
        for f in f_tiles:
            slope, silu, u = factors(0, span(f))
            f_v[0, :, span(f)] = u * slope
            f_v[1, :, span(f)] = silu
        wait(copies[:1])
        for f, copy in zip(f_tiles, downs):
            copy.wait()
            dh = dot(dy_v[0], wd_v[span(f), :], NT)
            store_grads(0, f, dh * f_v[0, :, span(f)], dh * f_v[1, :, span(f)])

    def first_hidden():
        for f in f_tiles:
            _, silu, u = factors(0, span(f))
            store_hidden(0, f, silu * u)
        start(load(2))

    def grads(k):
        slot = lax.rem(k, 2)
        wait(loaded(k))

        def rest(f, dh):
            slope, silu, u = factors(slot, span(f))
            store_hidden(k, f, silu * u)
            store_grads(k, f, dh * u * slope, dh * silu)

        dh = None
        for f in f_tiles:
            before, dh = dh, dot(dy_v[slot], wd_v[span(f), :], NT)
            if f:
                rest(f - WIDE, before)
        rest(f_tiles[-1], dh)

        @pl.when(k + 2 < chunks)
        def _():
            start(load(k + 2))

    def term(k, c, first=False):
        s, h = k // PARTS, lax.rem(k, PARTS)
        if first:
            weighted(c).wait()

        @pl.when(s > 0)
        def _():
            whole(buf.at[s, h, c], recv_sem.at[s - 1, h, c]).wait()

        cols = pl.ds(pl.multiple_of(c * width, width), width)
        rows = [dc_v[pl.ds(row_of(k, d), piece), :] for d in range(2)]
        acc = dot(jnp.concatenate(rows, axis=0), wc_v[cols, :], NT)
        for d in range(2):
            own = acc[d * piece:(d + 1) * piece]
            buf[s, h, c, d] = (own + buf[s, h, c, d].astype(F32)).astype(BF16)

        @pl.when(s < n - 1)
        def _():
            for d in range(2):
                hop(s, h, c, d).start()

        @pl.when(s == n - 1)
        def _():
            for d in range(2):
                spread(0, h, c, d).start()
                keep(0, h, c, d).start()

    first_grads()
    start(weight(1))
    pl.semaphore_wait(barrier, 2)
    term(0, 0, first=True)
    start(weight(2) + weight(3) + load(1))

    def term0(c, _):
        term(0, c, first=True)
        return 0

    lax.fori_loop(1, SUB, term0, 0)
    first_hidden()

    def terms(k):
        def body(c, _):
            term(k, c)
            return 0

        lax.fori_loop(0, SUB, body, 0)

    def chunk(k, _):
        grads(k)

        @pl.when(k < chunks - PARTS)
        def _():
            terms(k)
        return 0

    lax.fori_loop(1, chunks, chunk, 0)
    start([load_cols(dy, 0), load_cols(dy, 1)])

    def last_term(m, _):
        term(chunks - PARTS + m // SUB, lax.rem(m, SUB))
        slot = lax.rem(m, 2)
        load_cols(dy, m).wait()

        @pl.when(m >= 2)
        def _():
            save_dd(m - 2).wait()

        dd_v[slot] = dot(ht_v[...], x_v[slot], NN).astype(BF16)
        save_dd(m).start()

        @pl.when(m + 2 < messages)
        def _():
            load_cols(dy, m + 2).start()
        return 0

    lax.fori_loop(0, messages, last_term, 0)
    start([load_cols(x, 0), load_cols(x, 1)])

    def forward(r, m):
        h, c = m // SUB, lax.rem(m, SUB)
        whole(ag.at[r - 1, h, c], grecv_sem.at[r - 1, h, c]).wait()
        for d in range(2):
            spread(r, h, c, d).start()
            keep(r, h, c, d).start()

    per = -(-messages * (n - 3) // tiles)

    def tile(j, _):
        slot = lax.rem(j, 2)
        load_cols(x, j).wait()
        xt_v[...] = x_v[slot].T

        @pl.when(j >= 2)
        def _():
            wait(save_dw(j - 2))

        for i, (v, _) in enumerate(dws):
            for f in f_tiles:
                v[slot, :, span(f)] = dot(xt_v[...], dc_v[:, pl.ds(i * ff + f, min(WIDE, ff - f))], NN).astype(BF16)
        start(save_dw(j))

        @pl.when(j + 2 < tiles)
        def _():
            load_cols(x, j + 2).start()

        for r in range(1, n - 2):
            for i in range(per):
                m = j * per + i

                @pl.when(m < messages)
                def _():
                    forward(r, m)
        return 0

    lax.fori_loop(0, tiles, tile, 0)

    whole(buf.at[pl.ds(0, n - 1)], send_sem).wait()
    for r in range(n - 2):
        sent = buf.at[n - 1] if r == 0 else ag.at[r - 1]
        whole(sent, keep_sem.at[r]).wait()
        whole(sent, gsend_sem.at[r]).wait()
    for j in range(tiles - 2, tiles):
        save_dd(j).wait()
        wait(save_dw(j))
    for d, ref in enumerate((last_0, last_1)):
        whole(ref, end_sem.at[d]).wait()


def ring(n, x, dy, gate, up, w_gate, w_up, w_down):
    (rows, d), ff = dy.shape, gate.shape[1]
    piece, width = rows // (2 * n * PARTS), d // SUB
    assert TILE == 2 * piece
    assert n > 3 and d == PARTS * SUB * TILE
    dma = pltpu.SemaphoreType.DMA
    each = (PARTS, SUB, 2)
    return pl.pallas_call(
        functools.partial(ring_kernel, n),
        out_shape=[
            jax.ShapeDtypeStruct((rows, d), BF16),
            jax.ShapeDtypeStruct((PARTS * piece, d), BF16),
            jax.ShapeDtypeStruct((PARTS * piece, d), BF16),
            jax.ShapeDtypeStruct((d, ff), BF16),
            jax.ShapeDtypeStruct((d, ff), BF16),
            jax.ShapeDtypeStruct((ff, d), BF16),
        ],
        in_specs=[ANY] * 7,
        out_specs=[ANY] * 6,
        scratch_shapes=[
            pltpu.VMEM((ff, d), BF16),
            pltpu.VMEM((d, 2 * ff), BF16),
            pltpu.VMEM((2, 2 * piece, d), BF16),
            pltpu.VMEM((2, 2 * piece, ff), BF16),
            pltpu.VMEM((2, 2 * piece, ff), BF16),
            pltpu.VMEM((2, 2 * piece, ff), F32),
            pltpu.VMEM((ff, rows), BF16),
            pltpu.VMEM((rows, 2 * ff), BF16),
            pltpu.VMEM((n, *each, piece, width), BF16),
            pltpu.VMEM((n - 3, *each, piece, width), BF16),
            pltpu.VMEM((2, rows, TILE), BF16),
            pltpu.VMEM((TILE, rows), BF16),
            pltpu.VMEM((2, ff, TILE), BF16),
            dma((-(-ff // WIDE),)),
            dma((SUB,)),
            dma((3, 2)),
            dma(()),
            dma((n - 1, PARTS, SUB)),
            dma((n - 2,)),
            dma((n - 3, PARTS, SUB)),
            dma((2,)),
            dma((n - 2,)),
            dma((2,)),
            dma((2, 2)),
            dma((2,)),
        ],
        compiler_params=pltpu.CompilerParams(
            collective_id=0, has_side_effects=True, vmem_limit_bytes=62 * MIB
        ),
        cost_estimate=pl.CostEstimate(flops=12 * rows * d * ff, bytes_accessed=16 * rows * d, transcendentals=2 * rows * ff),
        name="ring",
    )(x, dy, gate, up, w_gate, w_up, w_down)


def finish_kernel(n, dx_in, last_0, last_1, dw_gate_in, dw_up_in, dw_down_in, dx, dw_gate, dw_up, dw_down,
                  dx_v, dg_v, du_v, dd_v, in_sem, out_sem):
    me, half = lax.axis_index("tp"), last_0.shape[0]
    moves = []
    for i in range(2 * (n - 1)):
        r, d = i // 2, i % 2
        rows = pl.ds(pl.multiple_of((2 * lax.rem(me + (2 * d - 1) * r + n, n) + d) * half, half), half)
        moves.append((dx_in.at[rows] if r < n - 2 else (last_0, last_1)[d], dx_v.at[i], dx.at[rows]))
    for i in range(COPIES):
        for src, v, dst in ((dw_gate_in, dg_v, dw_gate), (dw_up_in, du_v, dw_up), (dw_down_in, dd_v, dw_down)):
            rows = pl.ds(i * (v.shape[0] // COPIES), v.shape[0] // COPIES)
            moves.append((src.at[rows], v.at[rows], dst.at[rows]))
    bring = [pltpu.make_async_copy(a, b, in_sem.at[i]) for i, (a, b, _) in enumerate(moves)]
    put = [pltpu.make_async_copy(b, c, out_sem.at[i]) for i, (_, b, c) in enumerate(moves)]
    for copy in bring:
        copy.start()
    for copy, after in zip(bring, put):
        copy.wait()
        after.start()
    for copy in put:
        copy.wait()


def finish(n, dx, last_0, last_1, dw_gate, dw_up, dw_down):
    (rows, d), (ff, _) = dx.shape, dw_down.shape
    count = 2 * (n - 1) + 3 * COPIES
    dma = pltpu.SemaphoreType.DMA
    return pl.pallas_call(
        functools.partial(finish_kernel, n),
        out_shape=[jax.ShapeDtypeStruct(a.shape, a.dtype) for a in (dx, dw_gate, dw_up, dw_down)],
        in_specs=[ANY] * 6,
        out_specs=[ANY] * 4,
        scratch_shapes=[
            pltpu.VMEM((2 * (n - 1), *last_0.shape), BF16),
            *(pltpu.VMEM(a.shape, BF16) for a in (dw_gate, dw_up, dw_down)),
            dma((count,)),
            dma((count,)),
        ],
        compiler_params=pltpu.CompilerParams(vmem_limit_bytes=61 * MIB),
        cost_estimate=pl.CostEstimate(flops=2 * rows * d * ff, bytes_accessed=12 * rows * d, transcendentals=0),
        name="finish",
    )(dx, last_0, last_1, dw_gate, dw_up, dw_down)


def place_kernel(n, d, _, end, dx, sem):
    me, half = lax.axis_index("tp"), end.shape[0]
    row, part = (2 * lax.rem(me + (2 * d - 1) * (n - 1) + n, n) + d) * half, half // COPIES
    put = [
        pltpu.make_async_copy(
            end.at[pl.ds(i * part, part)], dx.at[pl.ds(pl.multiple_of(row + i * part, part), part)], sem
        )
        for i in range(COPIES)
    ]
    for copy in put:
        copy.start()
    pltpu.make_async_copy(end, end, sem).wait()


def place(n, d, dx, end):
    return pl.pallas_call(
        functools.partial(place_kernel, n, d),
        out_shape=jax.ShapeDtypeStruct(dx.shape, dx.dtype),
        in_specs=[ANY, pl.BlockSpec(memory_space=pltpu.VMEM)],
        out_specs=ANY,
        scratch_shapes=[pltpu.SemaphoreType.DMA(())],
        input_output_aliases={0: 0},
        compiler_params=pltpu.CompilerParams(vmem_limit_bytes=16 * MIB),
        name=f"place_{d}",
    )(dx, end)


def solution(mesh):
    n = mesh.shape["tp"]

    def step(x, dy, gate, up, w_gate, w_up, w_down):
        dx, *last, dw_gate, dw_up, dw_down = ring(n, x, dy, gate, up, w_gate, w_up, w_down)
        ends = [lax.ppermute(last[d], "tp", [(i, (i + 1 - 2 * d) % n) for i in range(n)]) for d in range(2)]
        dx, dw_gate, dw_up, dw_down = finish(n, dx, *last, dw_gate, dw_up, dw_down)
        for d in (1, 0):
            dx = place(n, d, dx, ends[d])
        return dx, dw_gate, dw_up, dw_down

    tokens, columns, rows = P("dp", None), P(None, "tp"), P("tp", None)
    return jax.shard_map(
        step,
        mesh=mesh,
        in_specs=(tokens, tokens, P("dp", "tp"), P("dp", "tp"), columns, columns, rows),
        out_specs=(tokens, P("dp", "tp"), P("dp", "tp"), P(("dp", "tp"), None)),
        check_vma=False,
    )
```
